128 devices in a mesh: lon: 8 (over y, core), lat: 16 (over x, z).
Axes of the slice: x: 4, y: 4, z: 4, core: 2. Of those that a mesh axis runs over, the one named last changes fastest.
Arguments:
- state_pert: bfloat16 [64, 32, 6, 128, 256], P('lon', 'lat'), may hold values from -6 to 6
- state_mean: float32 [64, 32, 6, 256], P('lon', 'lat'), may hold values from -6 to 6
- obs_anom: bfloat16 [24576, 128, 128], P(('lon', 'lat')), may hold values from -6 to 6
- innov: float32 [24576, 128], P(('lon', 'lat')), may hold values from -12 to 12
- obs_rinv: float32 [24576, 128], P(('lon', 'lat')), may hold values from 0.25 to 4
- obs_lon: int32 [24576, 128], P(('lon', 'lat')), may hold values from 0 to 1023, as said below
- obs_lat: int32 [24576, 128], P(('lon', 'lat')), may hold values from 40 to 471, as said below
- block_list: int32 [64, 32, 48], P('lon', 'lat'), may hold values from 0 to 24575, as said below
- block_count: int32 [64, 32], P('lon', 'lat'), may hold values from 6 to 48
Outputs:
- analysis: float32 [64, 32, 6, 128, 256], P('lon', 'lat')
The draws below stay inside these ranges and needn't reach their ends.
Inputs may be any that keep to these rules, and one draw needn't show every extreme that they name: `block_list`: block b is held by the device of flat index b // 192 over lon+lat. The first 48 entries of a patch's list name distinct blocks. Over all list entries of the patches of one device, each holder holds exactly 6 of the named blocks (counting repeats over patches). Only the first block_count entries of a patch's list are used. `obs_lon`: the longitude indices of one block's observations lie within 32 consecutive columns, counted around the periodic grid. `obs_lat`: the latitude indices of one block's observations lie within 32 consecutive columns.
All inputs are finite; a program needn't handle non-finite values.
Results may differ from the reference program's by a relative error of at most 0.0023.
Values may be sent and summed in bfloat16 or wider, within the bound.
A program may use at most 192 MiB of HBM per device.

```python
import math
import jax
import jax.numpy as jnp
from jax import lax

K = 128
PSIDE = 16
PLON = 8
PLAT = 2
LMAX = 48
OB = 128
SHARE = 4
NS_ITERS = 5
OBLK = 192
NPLON = 64
NPLAT = 32
NBLK = 24576
FIELDS = 6
COLS = 256
CAP = 6


def draw_innov(key, part):
    ramp = 1.0 + 2.0 * jnp.arange(NBLK, dtype=jnp.float32)[:, None] / (NBLK - 1)
    return jax.random.truncated_normal(key, -4.0, 4.0, (NBLK, OB), jnp.float32) * ramp


def block_layout(key):
    lon_devices = NPLON // PLON
    lat_devices = NPLAT // PLAT
    groups_lat = lat_devices // SHARE
    group_total = lon_devices * groups_lat
    slot_total = PLON * PLAT * LMAX
    scores = jax.random.randint(jax.random.fold_in(key, 7), (group_total, slot_total), 0, 1 << 20) * slot_total + jnp.arange(slot_total)[None, :]
    placed = jnp.argsort(scores, axis=1).astype(jnp.int32)
    holder = placed // CAP
    within = placed % CAP
    group_ids = jnp.arange(group_total, dtype=jnp.int32)[:, None]
    blocks = holder * OBLK + group_ids * CAP + within
    slot_ids = jnp.arange(slot_total, dtype=jnp.int32)[None, :]
    patch = slot_ids // LMAX
    patch_lon = patch // PLAT
    patch_lat = patch % PLAT
    group_lon = group_ids // groups_lat
    group_lat = group_ids % groups_lat
    centre_lon = (group_lon * PLON + patch_lon) * PSIDE + PSIDE // 2 + 0 * blocks
    centre_lat = group_lat * SHARE * PLAT * PSIDE + (SHARE - 1) * PLAT * PSIDE // 2 + patch_lat * PSIDE + PSIDE // 2 + 0 * blocks
    flat_blocks = blocks.reshape(-1)
    lon_of_block = jnp.zeros((NBLK,), jnp.int32).at[flat_blocks].set(centre_lon.reshape(-1))
    lat_of_block = jnp.zeros((NBLK,), jnp.int32).at[flat_blocks].set(centre_lat.reshape(-1))
    device_lon = jnp.arange(lon_devices, dtype=jnp.int32)[:, None]
    device_lat = jnp.arange(lat_devices, dtype=jnp.int32)[None, :]
    device_group = device_lon * groups_lat + device_lat // SHARE
    lists = blocks[device_group]
    lists = lists.reshape(lon_devices, lat_devices, PLON, PLAT, LMAX).transpose(0, 2, 1, 3, 4)
    return (lists.reshape(NPLON, NPLAT, LMAX).astype(jnp.int32), lon_of_block, lat_of_block)


def draw_block_list(key, part):
    lists, lon_of_block, lat_of_block = block_layout(key)
    return lists


def draw_obs_lon(key, part):
    lists, lon_of_block, lat_of_block = block_layout(key)
    offsets = jax.random.randint(jax.random.fold_in(key, 11), (NBLK, OB), 0, 32) - 16
    return ((lon_of_block[:, None] + offsets) % (NPLON * PSIDE)).astype(jnp.int32)


def draw_obs_lat(key, part):
    lists, lon_of_block, lat_of_block = block_layout(key)
    offsets = jax.random.randint(jax.random.fold_in(key, 13), (NBLK, OB), 0, 32) - 16
    column = jnp.arange(OB, dtype=jnp.int32)[None, :]
    offsets = jnp.where(column == 0, 15, jnp.where(column == 1, -16, offsets))
    return jnp.clip(lat_of_block[:, None] + offsets, 0, NPLAT * PSIDE - 1).astype(jnp.int32)


def touch_ends(entries, rng, smallest, high):
    longest = entries.shape.index(max(entries.shape))
    spots = []
    for shift in (0, 1):
        where = [jax.random.randint(jax.random.fold_in(rng, axis), (), 0, length) for axis, length in enumerate(entries.shape)]
        where[longest] = (where[longest] + shift) % entries.shape[longest]
        spots.append(tuple(where))
    return entries.at[spots[0]].set(smallest).at[spots[1]].set(high)


def block_scale(rng, extent, split, smallest, largest):
    def one(position, parts):
        steps = jax.random.uniform(jax.random.fold_in(jax.random.fold_in(rng, 6), position), (parts,), jnp.float32, smallest / len(split), largest / len(split))
        return jnp.repeat(jnp.exp(steps), extent[position] // parts).reshape((-1,) + (1,) * (len(extent) - position - 1))

    gain = one(*split[0])
    for cut in split[1:]:
        gain = gain * one(*cut)
    return gain


def centred(key, dims, scale, bound, pieces=(), held_as=jnp.bfloat16):
    loudness = block_scale(key, dims, pieces, -0.22, 0.18) if pieces else 1.0
    entries = jax.random.normal(key, dims, jnp.float32) * scale * loudness
    return jnp.minimum(jnp.maximum(entries, -bound), bound).astype(held_as)


def setup_inputs(seed: int = 0) -> dict:
    arg_keys = jax.random.split(jax.random.key(seed), 10)
    state_pert = centred(arg_keys[0], (NPLON, NPLAT, FIELDS, K, COLS), 1.0, 6.0, ((0, 8), (1, 16)))
    state_mean = centred(arg_keys[1], (NPLON, NPLAT, FIELDS, COLS), 1.0, 6.0, ((0, 8), (1, 16)), jnp.float32)
    obs_anom = centred(arg_keys[2], (NBLK, K, OB), 1.0, 6.0, ((0, 128),))
    innov = draw_innov(jax.random.fold_in(arg_keys[9], 71), 0)
    obs_rinv = jnp.clip(jnp.exp(math.log(4.0) - 2.7725887 * jax.random.uniform(arg_keys[4], (NBLK, OB), jnp.float32) ** block_scale(arg_keys[4], (NBLK, OB), ((0, 128),), -0.2, 0.2)), 0.25, 4.0)
    obs_lon = draw_obs_lon(jax.random.fold_in(arg_keys[9], 71), 0)
    obs_lat = draw_obs_lat(jax.random.fold_in(arg_keys[9], 71), 0)
    block_list = draw_block_list(jax.random.fold_in(arg_keys[9], 71), 0)
    block_count = touch_ends(jax.random.randint(arg_keys[8], (NPLON, NPLAT), CAP, LMAX + 1), jax.random.fold_in(arg_keys[8], 1), CAP, LMAX).astype(jnp.int32)
    return {"state_pert": state_pert, "state_mean": state_mean, "obs_anom": obs_anom, "innov": innov, "obs_rinv": obs_rinv, "obs_lon": obs_lon, "obs_lat": obs_lat, "block_list": block_list, "block_count": block_count}


loc_scale = 48.0

def product(left, right):
    return jnp.dot(left, right, precision=lax.Precision.HIGHEST)

def analyse(deviations, centre_state, anomalies, obs_fields, used_count, centre_lon, centre_lat, inflation, grid_lon):
    members = anomalies.shape[1]
    in_list = (jnp.arange(anomalies.shape[0]) < used_count).astype(jnp.float32)
    lon_gap = jnp.abs(obs_fields[:, 2] - centre_lon)
    lon_gap = jnp.minimum(lon_gap, grid_lon - lon_gap)
    lat_gap = obs_fields[:, 3] - centre_lat
    weight = obs_fields[:, 1] * jnp.exp(-(lon_gap * lon_gap + lat_gap * lat_gap) / (2.0 * loc_scale * loc_scale)) * in_list[:, None]
    scaled = (anomalies.astype(jnp.float32) * weight[:, None, :]).astype(jnp.bfloat16)
    gram_matrix = jnp.einsum('lko,lmo->km', scaled.astype(jnp.float32), anomalies.astype(jnp.float32))
    projected = jnp.einsum('lko,lo->k', scaled.astype(jnp.float32), obs_fields[:, 0], precision=lax.Precision.HIGHEST)
    identity = jnp.eye(members, dtype=jnp.float32)
    system = (members - 1) / inflation * identity + gram_matrix
    scaling = jnp.sqrt(jnp.sum(system * system))
    root = system / scaling
    inverse_root = identity
    for _ in range(NS_ITERS):
        factor = 1.5 * identity - 0.5 * product(inverse_root, root)
        root = product(root, factor)
        inverse_root = product(factor, inverse_root)
    inverse_sqrt = inverse_root / jnp.sqrt(scaling)
    mean_weights = product(inverse_sqrt, product(inverse_sqrt, projected[:, None]))
    weights = (jnp.sqrt(jnp.float32(members - 1)) * inverse_sqrt + mean_weights).astype(jnp.bfloat16)
    change = jnp.einsum('fjc,jk->fkc', deviations.astype(jnp.float32), weights.astype(jnp.float32))
    return centre_state[:, None, :] + change

def reference(state_pert, state_mean, obs_anom, innov, obs_rinv, obs_lon, obs_lat, block_list, block_count):
    members = obs_anom.shape[1]
    spread = lax.optimization_barrier(jnp.sum(jnp.square(obs_anom.astype(jnp.float32)), axis=1)) / (members - 1)
    inflation = jnp.sum(obs_rinv * innov * innov) / (jnp.sum(obs_rinv * spread) + NBLK * OB)
    obs_fields = jnp.stack([innov, obs_rinv, obs_lon.astype(jnp.float32), obs_lat.astype(jnp.float32)], axis=1)
    patch_total = NPLON * NPLAT
    patch_index = jnp.arange(patch_total)
    centre_lon = (patch_index // NPLAT * PSIDE).astype(jnp.float32) + (PSIDE - 1) / 2.0
    centre_lat = (patch_index % NPLAT * PSIDE).astype(jnp.float32) + (PSIDE - 1) / 2.0
    grid_lon = jnp.float32(NPLON * PSIDE)

    def patch_update(inputs):
        deviations, centre_state, block_ids, used_count, lon_centre, lat_centre = inputs
        return analyse(deviations, centre_state, obs_anom[block_ids], obs_fields[block_ids], used_count, lon_centre, lat_centre, inflation, grid_lon)
    inputs = (state_pert.reshape(patch_total, FIELDS, K, COLS), state_mean.reshape(patch_total, FIELDS, COLS), block_list.reshape(patch_total, LMAX).astype(jnp.int32), block_count.reshape(patch_total), centre_lon, centre_lat)
    updated = lax.map(patch_update, inputs)
    return updated.reshape(NPLON, NPLAT, FIELDS, K, COLS)
```

```python
import functools

import jax
import jax.numpy as jnp
from jax import lax
from jax.experimental import pallas as pl
from jax.experimental.pallas import tpu as pltpu
from jax.sharding import PartitionSpec as P

PSIDE = 16
NS_ITERS = 5
LOC_SCALE = 48.0
AXES = ("lon", "lat")
F32 = jnp.float32
BF16 = jnp.bfloat16


def totals_kernel(anom_ref, rinv_ref, innov_ref, out_ref, ext_ref):
    step = pl.program_id(0)
    blocks = anom_ref.shape[0]

    @pl.when(step == 0)
    def _():
        out_ref[...] = jnp.zeros_like(out_ref)

    innov = innov_ref[...]
    rinv = rinv_ref[...]
    high = innov.astype(BF16)
    rest = innov - high.astype(F32)
    mid = rest.astype(BF16)
    low = (rest - mid.astype(F32)).astype(BF16)
    ext = jnp.concatenate(
        [high[:, None, :].astype(F32), mid[:, None, :].astype(F32), low[:, None, :].astype(F32)]
        + [jnp.zeros((blocks, 13, innov.shape[1]), F32)],
        axis=1,
    )
    ext_ref[...] = ext.astype(BF16)
    out_ref[0:8, :] += jnp.sum((rinv * innov * innov).reshape(blocks // 8, 8, -1), axis=0)

    total = jnp.zeros((8, innov.shape[1]), F32)
    for b in range(blocks):
        a = anom_ref[b].astype(F32)
        squares = jnp.sum((a * a).reshape(-1, 8, a.shape[1]), axis=0)
        total = total + squares * rinv[b : b + 1, :]
    out_ref[8:16, :] += total


def gram_kernel(per, lat_devices, lon_patches, lat_patches, code_ref, anom_ref, ext_ref, rinv_ref,
                lon_ref, lat_ref, out_ref):
    count = out_ref.shape[0]
    first = pl.program_id(0) * count
    members = anom_ref.shape[1]
    half = members // 2
    grid_lon = float(8 * lon_patches * PSIDE)
    row = lax.broadcasted_iota(jnp.int32, (half, members), 0)
    lane = lax.broadcasted_iota(jnp.int32, (half, members), 1)
    keep = (lane >= half) | (row >= lane)
    on_diag = row == lane
    row8 = lax.broadcasted_iota(jnp.int32, (8, members), 0)

    def one(i, carry):
        who = first + i
        diags = jnp.zeros((8, members), F32)
        projs = jnp.zeros((8, members), F32)
        for s in range(per):
            code = code_ref[who * 8 + s]
            valid = code % 2
            patch = (code // 2) % 16
            held = code // 32
            cl = ((who // lat_devices) * lon_patches + patch // lat_patches) * PSIDE
            ct = ((who % lat_devices) * lat_patches + patch % lat_patches) * PSIDE
            cl = cl.astype(F32) + (PSIDE - 1) / 2.0
            ct = ct.astype(F32) + (PSIDE - 1) / 2.0
            gap = jnp.abs(lon_ref[pl.ds(held, 1), :] - cl)
            gap = jnp.minimum(gap, grid_lon - gap)
            other = lat_ref[pl.ds(held, 1), :] - ct
            weight = rinv_ref[pl.ds(held, 1), :] * jnp.exp(
                -(gap * gap + other * other) / (2.0 * LOC_SCALE * LOC_SCALE)
            )
            weight = weight * valid.astype(F32)
            a = anom_ref[held]
            scaled = (a.astype(F32) * weight).astype(BF16)
            left = jnp.concatenate([a, ext_ref[held]], axis=0)
            full = lax.dot_general(
                left, scaled, (((1,), (1,)), ((), ())), preferred_element_type=F32
            )
            top = full[:half, :]
            low = pltpu.roll(full[half:members, :], half, 1)
            out_ref[i, s * half : (s + 1) * half, :] = jnp.where(keep, top, low).astype(BF16)
            diag = jnp.sum(jnp.where(on_diag, low, 0.0), axis=0, keepdims=True)
            proj = jnp.sum(full[members : members + 8, :], axis=0, keepdims=True)
            diags = jnp.where(row8 == s, diag, diags)
            projs = jnp.where(row8 == s, proj, projs)
        high = projs.astype(BF16).astype(F32)
        extra = jnp.concatenate([diags, high, projs - high, jnp.zeros_like(high)], axis=0)
        out_ref[i, per * half : per * half + 32, :] = extra.astype(BF16)
        return carry

    lax.fori_loop(0, count, one, 0)


def gather_kernel(per, patch_ref, got_ref, acc_ref):
    count = got_ref.shape[0]
    step = pl.program_id(0)
    half = (got_ref.shape[1] - 32) // per

    @pl.when(step == 0)
    def _():
        acc_ref[...] = jnp.zeros_like(acc_ref)

    def one(i, carry):
        extra = got_ref[i, per * half :, :].astype(F32)
        proj = extra[8:16, :] + extra[16:24, :]
        for s in range(per):
            patch = patch_ref[(step * count + i) * per + s]
            acc_ref[patch, 0:half, :] += got_ref[i, s * half : (s + 1) * half, :].astype(F32)
            pair = jnp.concatenate(
                [extra[s : s + 1, :], proj[s : s + 1, :], jnp.zeros((6, proj.shape[1]), F32)], axis=0
            )
            acc_ref[patch, half : half + 8, :] += pair
        return carry

    lax.fori_loop(0, count, one, 0)


def halves(x):
    high = x.astype(BF16)
    return high, (x - high.astype(F32)).astype(BF16)


def product(left, right):
    n = right[0].shape[1]
    lhs = jnp.concatenate([left[0], left[1]], axis=1)
    upper = jnp.concatenate([right[0], right[1]], axis=1)
    lower = jnp.concatenate([right[0], jnp.zeros_like(right[1])], axis=1)
    both = jnp.dot(lhs, jnp.concatenate([upper, lower], axis=0), preferred_element_type=F32)
    return both[:, :n] + both[:, n:]


def update_kernel(base_ref, acc_ref, pert_ref, mean_ref, out_ref):
    count, fields, members, _ = pert_ref.shape
    half = members // 2
    row = lax.broadcasted_iota(jnp.int32, (members, members), 0)
    lane = lax.broadcasted_iota(jnp.int32, (members, members), 1)
    eye = jnp.where(row == lane, 1.0, 0.0)
    r = row[:half]
    c = lane[:half]
    base = base_ref[0]
    state = []
    for q in range(count):
        packed = acc_ref[q, 0:half, :]
        top = jnp.where((c >= half) | (r > c), packed, 0.0)
        low = pltpu.roll(jnp.where((c < half) & (r < c), packed, 0.0), half, 1)
        part = jnp.concatenate([top, low], axis=0)
        own = jnp.sum(jnp.where(r == c, packed, 0.0), axis=0, keepdims=True)
        own = own + pltpu.roll(acc_ref[q, half : half + 1, :], half, 1)
        system = part + part.T + jnp.where(row == lane, own + base, 0.0)
        scaling = jnp.sqrt(jnp.sum(jnp.sum(system * system, axis=0, keepdims=True), axis=1, keepdims=True))
        root = system / scaling
        factor = 1.5 * eye - 0.5 * root
        state.append([product(halves(root), halves(factor)), factor, scaling])
    for it in range(1, NS_ITERS):
        for q in range(count):
            root, inverse, _ = state[q]
            inverse2 = halves(inverse)
            factor = 1.5 * eye - 0.5 * product(inverse2, halves(root))
            factor2 = halves(factor)
            state[q][1] = product(factor2, inverse2)
            if it < NS_ITERS - 1:
                state[q][0] = product(factor2, halves(root))
    for q in range(count):
        _, inverse, scaling = state[q]
        inverse = inverse * (1.0 / jnp.sqrt(scaling))
        proj = acc_ref[q, half + 1 : half + 2, :]
        inverse2 = halves(inverse)
        mean = jnp.broadcast_to(proj, (8, members))
        mean = product(halves(mean), inverse2)
        mean = product(halves(mean), inverse2)[0:1, :]
        weights = (float(members - 1) ** 0.5 * inverse + mean).astype(BF16)
        for f in range(fields):
            change = jnp.dot(weights, pert_ref[q, f], preferred_element_type=F32)
            out_ref[q, f] = mean_ref[q, f : f + 1, :] + change


def on_device(
    state_pert, state_mean, obs_anom, innov, obs_rinv, obs_lon, obs_lat, block_list, block_count
):
    holders = lax.axis_size(AXES)
    lat_devices = lax.axis_size("lat")
    lon_patches, lat_patches, fields, members, columns = state_pert.shape
    patches = lon_patches * lat_patches
    list_length = block_list.shape[2]
    held_blocks, _, block_obs = obs_anom.shape
    slots = patches * list_length
    per = slots // holders
    half = members // 2
    rows = per * half + 32

    step_blocks = 16
    sums, ext = pl.pallas_call(
        totals_kernel,
        grid=(held_blocks // step_blocks,),
        in_specs=[
            pl.BlockSpec((step_blocks, members, block_obs), lambda i: (i, 0, 0)),
            pl.BlockSpec((step_blocks, block_obs), lambda i: (i, 0)),
            pl.BlockSpec((step_blocks, block_obs), lambda i: (i, 0)),
        ],
        out_specs=[
            pl.BlockSpec((16, block_obs), lambda i: (0, 0)),
            pl.BlockSpec((step_blocks, 16, block_obs), lambda i: (i, 0, 0)),
        ],
        out_shape=[
            jax.ShapeDtypeStruct((16, block_obs), F32),
            jax.ShapeDtypeStruct((held_blocks, 16, block_obs), BF16),
        ],
        name="totals",
    )(obs_anom, obs_rinv, innov)
    first_sum = jnp.sum(sums[0:8])
    second_sum = jnp.sum(sums[8:16]) / (members - 1)

    wanted = block_list.reshape(slots)
    holder = wanted // held_blocks
    slot = jnp.arange(slots)
    patch = slot // list_length
    valid = (slot % list_length < jnp.repeat(block_count.reshape(patches), list_length)).astype(jnp.int32)
    code = ((wanted % held_blocks) * 16 + patch) * 2 + valid
    earlier = (holder[:, None] == holder[None, :]) & (slot[None, :] < slot[:, None])
    rank = jnp.sum(earlier.astype(jnp.int32), axis=1)
    bucket = holder * per + rank
    requests = jnp.sum(jnp.where(bucket[:, None] == slot[None, :], code[:, None], 0), axis=0)
    message = jnp.concatenate(
        [
            requests.reshape(holders, per).astype(F32),
            jnp.broadcast_to(jnp.stack([first_sum, second_sum])[None, :], (holders, 2)),
        ],
        axis=1,
    )
    asked = lax.all_to_all(message, AXES, split_axis=0, concat_axis=0, tiled=True)
    total = jnp.sum(asked[:, per:], axis=0)
    inflation = total[0] / (total[1] + holders * held_blocks * block_obs)
    base = ((members - 1) / inflation).reshape(1)
    codes = asked.astype(jnp.int32).reshape(holders * 8)

    turn = 8
    whole3 = lambda i: (0, 0, 0)
    whole2 = lambda i: (0, 0)
    grams = pl.pallas_call(
        functools.partial(gram_kernel, per, lat_devices, lon_patches, lat_patches),
        grid=(holders // turn,),
        in_specs=[
            pl.BlockSpec(memory_space=pltpu.SMEM),
            pl.BlockSpec((held_blocks, members, block_obs), whole3),
            pl.BlockSpec((held_blocks, 16, block_obs), whole3),
            pl.BlockSpec((held_blocks, block_obs), whole2),
            pl.BlockSpec((held_blocks, block_obs), whole2),
            pl.BlockSpec((held_blocks, block_obs), whole2),
        ],
        out_specs=pl.BlockSpec((turn, rows, members), lambda i: (i, 0, 0)),
        out_shape=jax.ShapeDtypeStruct((holders, rows, members), BF16),
        name="grams",
    )(codes, obs_anom, ext, obs_rinv, obs_lon.astype(F32), obs_lat.astype(F32))

    got = lax.all_to_all(grams, AXES, split_axis=0, concat_axis=0, tiled=True)

    patch_of = (requests // 2) % 16
    acc = pl.pallas_call(
        functools.partial(gather_kernel, per),
        grid=(holders // turn,),
        in_specs=[
            pl.BlockSpec(memory_space=pltpu.SMEM),
            pl.BlockSpec((turn, rows, members), lambda i: (i, 0, 0)),
        ],
        out_specs=pl.BlockSpec((patches, half + 8, members), whole3),
        out_shape=jax.ShapeDtypeStruct((patches, half + 8, members), F32),
        name="gather",
    )(patch_of, got)

    pair = 2
    updated = pl.pallas_call(
        update_kernel,
        grid=(patches // pair,),
        in_specs=[
            pl.BlockSpec(memory_space=pltpu.SMEM),
            pl.BlockSpec((pair, half + 8, members), lambda i: (i, 0, 0)),
            pl.BlockSpec((pair, fields, members, columns), lambda i: (i, 0, 0, 0)),
            pl.BlockSpec((pair, fields, columns), lambda i: (i, 0, 0)),
        ],
        out_specs=pl.BlockSpec((pair, fields, members, columns), lambda i: (i, 0, 0, 0)),
        out_shape=jax.ShapeDtypeStruct((patches, fields, members, columns), F32),
        name="update",
    )(
        base,
        acc,
        state_pert.reshape(patches, fields, members, columns),
        state_mean.reshape(patches, fields, columns),
    )
    return updated.reshape(lon_patches, lat_patches, fields, members, columns)


def solution(mesh):
    in_specs = (
        P("lon", "lat", None, None, None),
        P("lon", "lat", None, None),
        P(AXES, None, None),
        P(AXES, None),
        P(AXES, None),
        P(AXES, None),
        P(AXES, None),
        P("lon", "lat", None),
        P("lon", "lat"),
    )
    out_specs = P("lon", "lat", None, None, None)
    return jax.shard_map(
        on_device, mesh=mesh, in_specs=in_specs, out_specs=out_specs, check_vma=False
    )
```

```python
import functools

import jax
import jax.numpy as jnp
from jax import lax
from jax.experimental import pallas as pl
from jax.experimental.pallas import tpu as pltpu
from jax.sharding import PartitionSpec as P

PSIDE = 16
NS_ITERS = 5
LOC_SCALE = 48.0
AXES = ("lon", "lat")
MESH = pl.DeviceIdType.MESH
F32 = jnp.float32
BF16 = jnp.bfloat16


def totals_kernel(anom_ref, rinv_ref, innov_ref, out_ref, ext_ref):
    step = pl.program_id(0)
    blocks = anom_ref.shape[0]

    @pl.when(step == 0)
    def _():
        out_ref[...] = jnp.zeros_like(out_ref)

    innov = innov_ref[...]
    rinv = rinv_ref[...]
    high = innov.astype(BF16)
    rest = innov - high.astype(F32)
    mid = rest.astype(BF16)
    low = (rest - mid.astype(F32)).astype(BF16)
    ext = jnp.concatenate(
        [high[:, None, :].astype(F32), mid[:, None, :].astype(F32), low[:, None, :].astype(F32)]
        + [jnp.zeros((blocks, 13, innov.shape[1]), F32)],
        axis=1,
    )
    ext_ref[...] = ext.astype(BF16)
    out_ref[0:8, :] += jnp.sum((rinv * innov * innov).reshape(blocks // 8, 8, -1), axis=0)

    total = jnp.zeros((8, innov.shape[1]), F32)
    for b in range(blocks):
        a = anom_ref[b].astype(F32)
        squares = jnp.sum((a * a).reshape(-1, 8, a.shape[1]), axis=0)
        total = total + squares * rinv[b : b + 1, :]
    out_ref[8:16, :] += total


def coordinates():
    lon, lat = lax.axis_index("lon"), lax.axis_index("lat")
    return lat // 4, lon // 2, lat % 4, lon % 2


def device_at(x, y, z, core):
    return (y * 2 + core, x * 4 + z)


def units_wait(ref, sem):
    pltpu.make_async_copy(ref, ref, sem).wait()


LINE_PEERS = [(0, 0, 0, 1)] + [
    tuple(step if axis == a else 0 for a in range(3)) + (core,)
    for axis in range(3)
    for step in (1, 2, 3)
    for core in (0, 1)
]
PLANE_PEERS = [
    (dx, dy, dz, 0)
    for dx in range(4)
    for dy in range(4)
    for dz in range(4)
    if 0 < (dx != 0) + (dy != 0) + (dz != 0) < 3
]


def shifted(me, offset):
    x, y, z, core = me
    dx, dy, dz, dc = offset
    return ((x + dx) % 4, (y + dy) % 4, (z + dz) % 4, (core + dc) % 2)


def greet(me, offsets):
    barrier = pltpu.get_barrier_semaphore()
    for offset in offsets:
        pl.semaphore_signal(
            barrier, inc=1, device_id=device_at(*shifted(me, offset)), device_id_type=MESH
        )
    pl.semaphore_wait(barrier, len(offsets))


def remote(src, dst, send, recv, target):
    return pltpu.make_async_remote_copy(
        src_ref=src,
        dst_ref=dst,
        send_sem=send,
        recv_sem=recv,
        device_id=device_at(*target),
        device_id_type=MESH,
    )


def gram_kernel(per, lon_patches, lat_patches, code_ref, table_ref, anom_ref, ext_ref, rinv_ref,
                lon_ref, lat_ref, got_ref, codes_ref, stage, send, recv, own, send2, recv2, own2):
    me = coordinates()
    xm, ym, zm, cm = me
    mine = (zm, xm, ym)
    members = anom_ref.shape[1]
    half = members // 2
    third = (half + 8) // 3
    requesters = stage.shape[0]
    grid_lon = float(8 * lon_patches * PSIDE)
    row = lax.broadcasted_iota(jnp.int32, (half, members), 0)
    lane = lax.broadcasted_iota(jnp.int32, (half, members), 1)
    keep = (lane >= half) | (row >= lane)
    on_diag = row == lane
    row8 = lax.broadcasted_iota(jnp.int32, (8, members), 0)

    greet(me, LINE_PEERS)
    for q in range(3):
        source = mine[q] * 2 + cm
        for step in range(4):
            for core in range(2):
                offset = [0, 0, 0, core]
                offset[(2, 0, 1)[q]] = step
                dst = codes_ref.at[q, source]
                if step == 0 and core == 0:
                    pltpu.make_async_copy(table_ref, dst, own2.at[q]).start()
                else:
                    remote(table_ref, dst, send2, recv2, shifted(me, offset)).start()

    def offset_of(i):
        dx = i % 4
        dy = (i + i // 4) % 4
        dz = (i + i // 16) % 4
        return dx, dy, dz, i // 64

    def ship(i):
        dx, dy, dz, dc = offset_of(i)
        x, y, z, core = shifted(me, (dx, dy, dz, dc))
        targets = ((xm, ym, z, core), (x, ym, zm, core), (xm, y, zm, core))
        places = (x * 4 + y, y * 4 + z, x * 4 + z)
        for q, moved in enumerate((dz, dx, dy)):
            src = stage.at[i, q]
            dst = got_ref.at[q, mine[q] * 2 + cm, places[q]]
            stays = (moved == 0) & (dc == 0)

            @pl.when(stays)
            def _():
                pltpu.make_async_copy(src, dst, own).start()

            @pl.when(jnp.logical_not(stays))
            def _():
                remote(src, dst, send, recv, targets[q]).start()

    def one(i, carry):
        x, y, z, core = shifted(me, offset_of(i))
        lon_device = y * 2 + core
        lat_device = x * 4 + z
        who = lon_device * 16 + lat_device
        pieces = []
        for s in range(per):
            code = code_ref[who * 8 + s]
            valid = code % 2
            patch = (code // 2) % 16
            held = code // 32
            cl = (lon_device * lon_patches + patch // lat_patches) * PSIDE
            ct = (lat_device * lat_patches + patch % lat_patches) * PSIDE
            cl = cl.astype(F32) + (PSIDE - 1) / 2.0
            ct = ct.astype(F32) + (PSIDE - 1) / 2.0
            gap = jnp.abs(lon_ref[pl.ds(held, 1), :] - cl)
            gap = jnp.minimum(gap, grid_lon - gap)
            other = lat_ref[pl.ds(held, 1), :] - ct
            weight = rinv_ref[pl.ds(held, 1), :] * jnp.exp(
                -(gap * gap + other * other) / (2.0 * LOC_SCALE * LOC_SCALE)
            )
            weight = weight * valid.astype(F32)
            a = anom_ref[held]
            scaled = (a.astype(F32) * weight).astype(BF16)
            left = jnp.concatenate([a, ext_ref[held]], axis=0)
            full = lax.dot_general(
                left, scaled, (((1,), (1,)), ((), ())), preferred_element_type=F32
            )
            top = full[:half, :]
            low = pltpu.roll(full[half:members, :], half, 1)
            diag = jnp.sum(jnp.where(on_diag, low, 0.0), axis=0, keepdims=True)
            proj = jnp.sum(full[members : members + 8, :], axis=0, keepdims=True)
            high = proj.astype(BF16).astype(F32)
            extra = jnp.where(
                row8 == 0, diag, jnp.where(row8 == 1, high, jnp.where(row8 == 2, proj - high, 0.0))
            )
            pieces.append(jnp.concatenate([jnp.where(keep, top, low), extra], axis=0))
        for q in range(3):
            for s in range(0, per, 2):
                both = jnp.concatenate(
                    [pieces[s][q * third : (q + 1) * third], pieces[s + 1][q * third : (q + 1) * third]],
                    axis=0,
                )
                stage[i, q, s * third : (s + 2) * third, :] = both.astype(BF16)

        @pl.when(i > 0)
        def _():
            ship(i - 1)

        return carry

    lax.fori_loop(0, requesters, one, 0)
    ship(requesters - 1)

    for q in range(3):
        pltpu.make_async_copy(table_ref, codes_ref.at[q, 0], own2.at[q]).wait()
    units_wait(codes_ref.at[:, 0:7], send2)
    units_wait(codes_ref.at[:, 0:7], recv2)
    units_wait(stage.at[0:16], own)
    units_wait(stage.at[0:112], send)
    units_wait(got_ref.at[:, 0:7], recv)


def add_kernel(per, me_ref, codes_ref, got_ref, out_ref, acc):
    q = pl.program_id(0)
    place = pl.program_id(1)
    major, minor = place // 4, place % 4
    x = jnp.where(q == 1, me_ref[0], major)
    y = jnp.where(q == 2, me_ref[1], jnp.where(q == 0, minor, major))
    z = jnp.where(q == 0, me_ref[2], minor)
    who = (y * 2 + me_ref[3]) * 16 + x * 4 + z
    third = got_ref.shape[3] // per
    acc[...] = jnp.zeros_like(acc)
    for source in range(got_ref.shape[1]):
        for s in range(0, per, 2):
            both = got_ref[0, source, 0, s * third : (s + 2) * third, :].astype(F32)
            for t in range(2):
                where = who * 8 + s + t
                code = codes_ref[0, source * 8 + where // 128, where % 128]
                start = pl.multiple_of(((code // 2) % 16) * third, 8)
                acc[pl.ds(start, third), :] += both[t * third : (t + 1) * third]

    @pl.when(q == 2)
    def _():
        row8 = lax.broadcasted_iota(jnp.int32, (8, acc.shape[1]), 0)
        for p in range(acc.shape[0] // third):
            rows = acc[p * third + 16 : p * third + 24, :]
            proj = rows[1:2, :] + rows[2:3, :]
            high = proj.astype(BF16).astype(F32)
            acc[p * third + 16 : p * third + 24, :] = jnp.where(
                row8 == 1, high, jnp.where(row8 == 2, proj - high, rows)
            )

    out_ref[0, 0] = acc[...].astype(BF16)


def plane_kernel(dense_ref, acc_ref, held, send, recv, own):
    me = coordinates()
    xm, ym, zm, cm = me
    places = (xm * 4 + ym, ym * 4 + zm, xm * 4 + zm)
    third = dense_ref.shape[2] // acc_ref.shape[0]
    greet(me, PLANE_PEERS)
    for k in range(16):
        first, second = k % 4, (k + k // 4) % 4
        for q in range(3):
            offset = ((first, second, 0, 0), (0, first, second, 0), (first, 0, second, 0))[q]
            x, y, z, core = shifted(me, offset)
            place = (x * 4 + y, y * 4 + z, x * 4 + z)[q]
            src = dense_ref.at[q, place]
            dst = held.at[q, places[q]]
            if first == 0 and second == 0:
                pltpu.make_async_copy(src, dst, own.at[q]).start()
            else:
                remote(src, dst, send, recv.at[q], (x, y, z, core)).start()
    for q in range(3):
        pltpu.make_async_copy(dense_ref.at[q, 0], held.at[q, 0], own.at[q]).wait()
        units_wait(held.at[q, 0:15], recv.at[q])

        def one(j, carry):
            start = pl.multiple_of(j * 2 * third, 16)
            total = held[q, 0, pl.ds(start, 2 * third), :].astype(F32)
            for source in range(1, 16):
                total += held[q, source, pl.ds(start, 2 * third), :].astype(F32)
            acc_ref[2 * j, q * third : (q + 1) * third, :] = total[:third]
            acc_ref[2 * j + 1, q * third : (q + 1) * third, :] = total[third:]
            return carry

        lax.fori_loop(0, acc_ref.shape[0] // 2, one, 0)
    units_wait(held.at[:, 0:15], send)


def halves(x):
    high = x.astype(BF16)
    return high, (x - high.astype(F32)).astype(BF16)


def product(left, right):
    n = right[0].shape[1]
    lhs = jnp.concatenate([left[0], left[1]], axis=1)
    upper = jnp.concatenate([right[0], right[1]], axis=1)
    lower = jnp.concatenate([right[0], jnp.zeros_like(right[1])], axis=1)
    both = jnp.dot(lhs, jnp.concatenate([upper, lower], axis=0), preferred_element_type=F32)
    return both[:, :n] + both[:, n:]


def update_kernel(base_ref, acc_ref, pert_ref, mean_ref, out_ref):
    count, fields, members, _ = pert_ref.shape
    half = members // 2
    row = lax.broadcasted_iota(jnp.int32, (members, members), 0)
    lane = lax.broadcasted_iota(jnp.int32, (members, members), 1)
    eye = jnp.where(row == lane, 1.0, 0.0)
    r = row[:half]
    c = lane[:half]
    base = base_ref[0]
    state = []
    for q in range(count):
        packed = acc_ref[q, 0:half, :]
        top = jnp.where((c >= half) | (r > c), packed, 0.0)
        low = pltpu.roll(jnp.where((c < half) & (r < c), packed, 0.0), half, 1)
        part = jnp.concatenate([top, low], axis=0)
        own = jnp.sum(jnp.where(r == c, packed, 0.0), axis=0, keepdims=True)
        own = own + pltpu.roll(acc_ref[q, half : half + 1, :], half, 1)
        system = part + part.T + jnp.where(row == lane, own + base, 0.0)
        scaling = jnp.sqrt(jnp.sum(jnp.sum(system * system, axis=0, keepdims=True), axis=1, keepdims=True))
        root = system / scaling
        factor = 1.5 * eye - 0.5 * root
        state.append([product(halves(root), halves(factor)), factor, scaling])
    for it in range(1, NS_ITERS):
        for q in range(count):
            root, inverse, _ = state[q]
            inverse2 = halves(inverse)
            factor = 1.5 * eye - 0.5 * product(inverse2, halves(root))
            factor2 = halves(factor)
            state[q][1] = product(factor2, inverse2)
            if it < NS_ITERS - 1:
                state[q][0] = product(factor2, halves(root))
    for q in range(count):
        _, inverse, scaling = state[q]
        inverse = inverse * (1.0 / jnp.sqrt(scaling))
        proj = acc_ref[q, half + 1 : half + 2, :] + acc_ref[q, half + 2 : half + 3, :]
        inverse2 = halves(inverse)
        mean = jnp.broadcast_to(proj, (8, members))
        mean = product(halves(mean), inverse2)
        mean = product(halves(mean), inverse2)[0:1, :]
        weights = (float(members - 1) ** 0.5 * inverse + mean).astype(BF16)
        for f in range(fields):
            change = jnp.dot(weights, pert_ref[q, f], preferred_element_type=F32)
            out_ref[q, f] = mean_ref[q, f : f + 1, :] + change


def on_device(
    state_pert, state_mean, obs_anom, innov, obs_rinv, obs_lon, obs_lat, block_list, block_count
):
    holders = lax.axis_size(AXES)
    lon_patches, lat_patches, fields, members, columns = state_pert.shape
    patches = lon_patches * lat_patches
    list_length = block_list.shape[2]
    held_blocks, _, block_obs = obs_anom.shape
    slots = patches * list_length
    per = slots // holders
    half = members // 2

    step_blocks = 16
    sums, ext = pl.pallas_call(
        totals_kernel,
        grid=(held_blocks // step_blocks,),
        in_specs=[
            pl.BlockSpec((step_blocks, members, block_obs), lambda i: (i, 0, 0)),
            pl.BlockSpec((step_blocks, block_obs), lambda i: (i, 0)),
            pl.BlockSpec((step_blocks, block_obs), lambda i: (i, 0)),
        ],
        out_specs=[
            pl.BlockSpec((16, block_obs), lambda i: (0, 0)),
            pl.BlockSpec((step_blocks, 16, block_obs), lambda i: (i, 0, 0)),
        ],
        out_shape=[
            jax.ShapeDtypeStruct((16, block_obs), F32),
            jax.ShapeDtypeStruct((held_blocks, 16, block_obs), BF16),
        ],
        name="totals",
    )(obs_anom, obs_rinv, innov)
    first_sum = jnp.sum(sums[0:8])
    second_sum = jnp.sum(sums[8:16]) / (members - 1)

    wanted = block_list.reshape(slots)
    holder = wanted // held_blocks
    slot = jnp.arange(slots)
    patch = slot // list_length
    valid = (slot % list_length < jnp.repeat(block_count.reshape(patches), list_length)).astype(jnp.int32)
    code = ((wanted % held_blocks) * 16 + patch) * 2 + valid
    earlier = (holder[:, None] == holder[None, :]) & (slot[None, :] < slot[:, None])
    rank = jnp.sum(earlier.astype(jnp.int32), axis=1)
    bucket = holder * per + rank
    requests = jnp.sum(jnp.where(bucket[:, None] == slot[None, :], code[:, None], 0), axis=0)
    message = jnp.concatenate(
        [
            requests.reshape(holders, per).astype(F32),
            jnp.broadcast_to(jnp.stack([first_sum, second_sum])[None, :], (holders, 2)),
        ],
        axis=1,
    )
    asked = lax.all_to_all(message, AXES, split_axis=0, concat_axis=0, tiled=True)
    total = jnp.sum(asked[:, per:], axis=0)
    inflation = total[0] / (total[1] + holders * held_blocks * block_obs)
    base = ((members - 1) / inflation).reshape(1)
    codes = asked.astype(jnp.int32).reshape(holders * 8)

    third = (half + 8) // 3
    got, tables = pl.pallas_call(
        functools.partial(gram_kernel, per, lon_patches, lat_patches),
        in_specs=[pl.BlockSpec(memory_space=pltpu.SMEM), pl.BlockSpec(memory_space=pl.ANY)]
        + [pl.BlockSpec(memory_space=pltpu.VMEM)] * 5,
        out_specs=[pl.BlockSpec(memory_space=pl.ANY)] * 2,
        out_shape=[
            jax.ShapeDtypeStruct((3, 8, 16, per * third, members), BF16),
            jax.ShapeDtypeStruct((3, 8, 8, 128), jnp.int32),
        ],
        scratch_shapes=[
            pltpu.VMEM((holders, 3, per * third, members), BF16),
            pltpu.SemaphoreType.DMA,
            pltpu.SemaphoreType.DMA,
            pltpu.SemaphoreType.DMA,
            pltpu.SemaphoreType.DMA,
            pltpu.SemaphoreType.DMA,
            pltpu.SemaphoreType.DMA((3,)),
        ],
        compiler_params=pltpu.CompilerParams(collective_id=0, has_side_effects=True),
        name="grams",
    )(codes, codes.reshape(8, 128), obs_anom, ext, obs_rinv, obs_lon.astype(F32), obs_lat.astype(F32))

    x, y, z, core = coordinates()
    dense = pl.pallas_call(
        functools.partial(add_kernel, per),
        grid=(3, 16),
        in_specs=[
            pl.BlockSpec(memory_space=pltpu.SMEM),
            pl.BlockSpec((1, 64, 128), lambda q, i: (q, 0, 0), memory_space=pltpu.SMEM),
            pl.BlockSpec((1, 8, 1, per * third, members), lambda q, i: (q, 0, i, 0, 0)),
        ],
        out_specs=pl.BlockSpec((1, 1, patches * third, members), lambda q, i: (q, i, 0, 0)),
        out_shape=jax.ShapeDtypeStruct((3, 16, patches * third, members), BF16),
        scratch_shapes=[pltpu.VMEM((patches * third, members), F32)],
        name="adds",
    )(jnp.stack([x, y, z, core]), tables.reshape(3, 64, 128), got)

    acc = pl.pallas_call(
        plane_kernel,
        in_specs=[pl.BlockSpec(memory_space=pl.ANY)],
        out_specs=pl.BlockSpec(memory_space=pltpu.VMEM),
        out_shape=jax.ShapeDtypeStruct((patches, half + 8, members), F32),
        scratch_shapes=[
            pltpu.VMEM((3, 16, patches * third, members), BF16),
            pltpu.SemaphoreType.DMA,
            pltpu.SemaphoreType.DMA((3,)),
            pltpu.SemaphoreType.DMA((3,)),
        ],
        compiler_params=pltpu.CompilerParams(collective_id=1, has_side_effects=True),
        name="planes",
    )(dense)

    pair = 2
    updated = pl.pallas_call(
        update_kernel,
        grid=(patches // pair,),
        in_specs=[
            pl.BlockSpec(memory_space=pltpu.SMEM),
            pl.BlockSpec((pair, half + 8, members), lambda i: (i, 0, 0)),
            pl.BlockSpec((pair, fields, members, columns), lambda i: (i, 0, 0, 0)),
            pl.BlockSpec((pair, fields, columns), lambda i: (i, 0, 0)),
        ],
        out_specs=pl.BlockSpec((pair, fields, members, columns), lambda i: (i, 0, 0, 0)),
        out_shape=jax.ShapeDtypeStruct((patches, fields, members, columns), F32),
        name="update",
    )(
        base,
        acc,
        state_pert.reshape(patches, fields, members, columns),
        state_mean.reshape(patches, fields, columns),
    )
    return updated.reshape(lon_patches, lat_patches, fields, members, columns)


def solution(mesh):
    in_specs = (
        P("lon", "lat", None, None, None),
        P("lon", "lat", None, None),
        P(AXES, None, None),
        P(AXES, None),
        P(AXES, None),
        P(AXES, None),
        P(AXES, None),
        P("lon", "lat", None),
        P("lon", "lat"),
    )
    out_specs = P("lon", "lat", None, None, None)
    return jax.shard_map(
        on_device, mesh=mesh, in_specs=in_specs, out_specs=out_specs, check_vma=False
    )
```

```python
import functools

import jax
import jax.numpy as jnp
from jax import lax
from jax.experimental import pallas as pl
from jax.experimental.pallas import tpu as pltpu
from jax.sharding import PartitionSpec as P

PSIDE = 16
NS_ITERS = 5
LOC_SCALE = 48.0
AXES = ("lon", "lat")
MESH = pl.DeviceIdType.MESH
CHAINS = 2
PAIR = 8
F32 = jnp.float32
BF16 = jnp.bfloat16


def totals_kernel(turn, anom_ref, rinv_ref, innov_ref, out_ref, ext_ref, held, sems):
    blocks, _, width = anom_ref.shape
    turns = blocks // turn

    def copy(k):
        return pltpu.make_async_copy(
            anom_ref.at[pl.ds(k * turn, turn)], held.at[pl.ds(k * turn, turn)], sems.at[k]
        )

    for k in range(turns):
        copy(k).start()
    innov = innov_ref[...]
    high = innov.astype(BF16).astype(F32)
    rest = innov - high
    mid = rest.astype(BF16).astype(F32)
    low = rest - mid
    ext = jnp.concatenate(
        [high[:, None, :], mid[:, None, :], low[:, None, :], jnp.zeros((blocks, 13, width), F32)], axis=1
    )
    ext_ref[...] = ext.astype(BF16)
    out_ref[0:8, :] = jnp.sum((rinv_ref[...] * innov * innov).reshape(blocks // 8, 8, width), axis=0)

    def one(k, total):
        copy(k).wait()
        first = pl.multiple_of(k * turn, turn)
        rinv = rinv_ref[pl.ds(first, turn), :]
        for b in range(turn):
            a = held[first + b].astype(F32)
            squares = jnp.sum((a * a).reshape(-1, 8, width), axis=0)
            total = total + squares * rinv[b : b + 1, :]
        return total

    out_ref[8:16, :] = lax.fori_loop(0, turns, one, jnp.zeros((8, width), F32))


def coordinates():
    lon, lat = lax.axis_index("lon"), lax.axis_index("lat")
    return lax.div(lat, 4), lax.div(lon, 2), lax.rem(lat, 4), lax.rem(lon, 2)


def device_at(x, y, z, core):
    return (y * 2 + core, x * 4 + z)


def units_wait(ref, sem):
    pltpu.make_async_copy(ref, ref, sem).wait()


LINE_PEERS = [(0, 0, 0, 1)] + [
    tuple(step if axis == a else 0 for a in range(3)) + (core,)
    for axis in range(3)
    for step in (1, 2, 3)
    for core in (0, 1)
]
PLANE_PEERS = [
    (dx, dy, dz, 0)
    for dx in range(4)
    for dy in range(4)
    for dz in range(4)
    if 0 < (dx != 0) + (dy != 0) + (dz != 0) < 3
]


def shifted(me, offset):
    x, y, z, core = me
    dx, dy, dz, dc = offset
    return tuple(
        lax.rem(a + d, n) if not isinstance(d, int) or d else a
        for a, d, n in ((x, dx, 4), (y, dy, 4), (z, dz, 4), (core, dc, 2))
    )


def greet(me, offsets):
    barrier = pltpu.get_barrier_semaphore()
    for offset in offsets:
        pl.semaphore_signal(
            barrier, inc=1, device_id=device_at(*shifted(me, offset)), device_id_type=MESH
        )
    pl.semaphore_wait(barrier, len(offsets))


def remote(src, dst, send, recv, target):
    return pltpu.make_async_remote_copy(
        src_ref=src,
        dst_ref=dst,
        send_sem=send,
        recv_sem=recv,
        device_id=device_at(*target),
        device_id_type=MESH,
    )


def gram_kernel(per, lon_patches, lat_patches, code_ref, table_ref, anom_ref, ext_ref, rinv_ref,
                lon_ref, lat_ref, got_ref, codes_ref, stage, send, recv, own, send2, recv2, own2):
    me = coordinates()
    xm, ym, zm, cm = me
    mine = (zm, xm, ym)
    members = anom_ref.shape[1]
    half = members // 2
    third = (half + 8) // 3
    requesters = stage.shape[0]
    grid_lon = float(8 * lon_patches * PSIDE)
    row = lax.broadcasted_iota(jnp.int32, (half, members), 0)
    lane = lax.broadcasted_iota(jnp.int32, (half, members), 1)
    keep = (lane >= half) | (row >= lane)
    on_diag = row == lane
    row8 = lax.broadcasted_iota(jnp.int32, (8, members), 0)

    greet(me, LINE_PEERS)
    for q in range(3):
        source = mine[q] * 2 + cm
        for step in range(4):
            for core in range(2):
                offset = [0, 0, 0, core]
                offset[(2, 0, 1)[q]] = step
                dst = codes_ref.at[q, source]
                if step == 0 and core == 0:
                    pltpu.make_async_copy(table_ref, dst, own2.at[q]).start()
                else:
                    remote(table_ref, dst, send2, recv2, shifted(me, offset)).start()

    def offset_of(i):
        dx = lax.rem(i, 4)
        dy = lax.rem(i + lax.div(i, 4), 4)
        dz = lax.rem(i + lax.div(i, 16), 4)
        return dx, dy, dz, lax.div(i, 64)

    def ship(i):
        dx, dy, dz, dc = offset_of(i)
        x, y, z, core = shifted(me, (dx, dy, dz, dc))
        targets = ((xm, ym, z, core), (x, ym, zm, core), (xm, y, zm, core))
        places = (x * 4 + y, y * 4 + z, x * 4 + z)
        for q, moved in enumerate((dz, dx, dy)):
            src = stage.at[i, q]
            dst = got_ref.at[q, mine[q] * 2 + cm, places[q]]
            stays = (moved == 0) & (dc == 0)

            @pl.when(stays)
            def _():
                pltpu.make_async_copy(src, dst, own).start()

            @pl.when(jnp.logical_not(stays))
            def _():
                remote(src, dst, send, recv, targets[q]).start()

    def one(i, carry):
        x, y, z, core = shifted(me, offset_of(i))
        lon_device = y * 2 + core
        lat_device = x * 4 + z
        who8 = (lon_device * 16 + lat_device) * 8
        lon_first = lon_device * (lon_patches * PSIDE)
        lat_first = lat_device * (lat_patches * PSIDE)
        pieces = []
        for s in range(per):
            code = code_ref[who8 + s]
            valid = code & 1
            held = code >> 8
            cl = (lon_first + (code & 112)).astype(F32) + (PSIDE - 1) / 2.0
            ct = (lat_first + ((code & 128) >> 3)).astype(F32) + (PSIDE - 1) / 2.0
            gap = jnp.abs(lon_ref[pl.ds(held, 1), :] - cl)
            gap = jnp.minimum(gap, grid_lon - gap)
            other = lat_ref[pl.ds(held, 1), :] - ct
            weight = rinv_ref[pl.ds(held, 1), :] * jnp.exp(
                -(gap * gap + other * other) / (2.0 * LOC_SCALE * LOC_SCALE)
            )
            weight = weight * valid.astype(F32)
            a = anom_ref[held]
            scaled = (a.astype(F32) * weight).astype(BF16)
            left = jnp.concatenate([a, ext_ref[held]], axis=0)
            full = lax.dot_general(
                left, scaled, (((1,), (1,)), ((), ())), preferred_element_type=F32
            )
            top = full[:half, :]
            low = pltpu.roll(full[half:members, :], half, 1)
            diag = jnp.sum(jnp.where(on_diag, low, 0.0), axis=0, keepdims=True)
            proj = jnp.sum(full[members : members + 8, :], axis=0, keepdims=True)
            high = proj.astype(BF16).astype(F32)
            extra = jnp.where(
                row8 == 0, diag, jnp.where(row8 == 1, high, jnp.where(row8 == 2, proj - high, 0.0))
            )
            pieces.append(jnp.concatenate([jnp.where(keep, top, low), extra], axis=0))
        for q in range(3):
            for s in range(0, per, 2):
                both = jnp.concatenate(
                    [pieces[s][q * third : (q + 1) * third], pieces[s + 1][q * third : (q + 1) * third]],
                    axis=0,
                )
                stage[i, q, s * third : (s + 2) * third, :] = both.astype(BF16)

        @pl.when(i > 0)
        def _():
            ship(i - 1)

        return carry

    lax.fori_loop(0, requesters, one, 0)
    ship(jnp.int32(requesters - 1))

    for q in range(3):
        pltpu.make_async_copy(table_ref, codes_ref.at[q, 0], own2.at[q]).wait()
    units_wait(codes_ref.at[:, 0:7], send2)
    units_wait(codes_ref.at[:, 0:7], recv2)
    units_wait(stage.at[0:16], own)
    units_wait(stage.at[0:112], send)
    units_wait(got_ref.at[:, 0:7], recv)


def add_kernel(per, me_ref, starts_ref, got_ref, out_ref, held, made, sems, out_sems, *accs):
    sources, places = held.shape[1:3]
    third = held.shape[3] // per
    chains = len(accs)
    row8 = lax.broadcasted_iota(jnp.int32, (8, held.shape[4]), 0)

    def copy(q, source):
        return pltpu.make_async_copy(got_ref.at[q, source], held.at[q, source], sems.at[q, source])

    for q in range(3):
        for source in range(sources):
            copy(q, source).start()
    for q in range(3):
        for source in range(sources):
            copy(q, source).wait()

        def one(place, carry):
            major, minor = lax.div(place, 4), lax.rem(place, 4)
            x = me_ref[0] if q == 1 else major
            y = me_ref[1] if q == 2 else (minor if q == 0 else major)
            z = me_ref[2] if q == 0 else minor
            first = ((y * 2 + me_ref[3]) * 16 + x * 4 + z) * 8
            for acc in accs:
                acc[...] = jnp.zeros_like(acc)
            for source in range(sources):
                for s in range(0, per, 2):
                    both = held[q, source, place, s * third : (s + 2) * third, :].astype(F32)
                    for t in range(2):
                        start = pl.multiple_of(starts_ref[q, source, first + s + t], 8)
                        accs[(s + t) % chains][pl.ds(start, third), :] += both[t * third : (t + 1) * third]
            if q < 2:
                made[q, place] = functools.reduce(lambda a, b: a + b, [acc[...] for acc in accs]).astype(BF16)
            else:
                for p in range(0, accs[0].shape[0] // third, 2):
                    rows = slice(p * third, (p + 2) * third)
                    total = functools.reduce(lambda a, b: a + b, [acc[rows, :] for acc in accs])
                    parts = []
                    for t in range(2):
                        top = total[t * third : t * third + 16]
                        last = total[t * third + 16 : (t + 1) * third]
                        proj = last[1:2, :] + last[2:3, :]
                        high = proj.astype(BF16).astype(F32)
                        parts += [top, jnp.where(row8 == 1, high, jnp.where(row8 == 2, proj - high, last))]
                    made[q, place, rows, :] = jnp.concatenate(parts, axis=0).astype(BF16)
            return carry

        lax.fori_loop(0, places, one, 0)
        pltpu.make_async_copy(made.at[q], out_ref.at[q], out_sems.at[q]).start()
    for q in range(3):
        pltpu.make_async_copy(made.at[q], out_ref.at[q], out_sems.at[q]).wait()


def plane_kernel(dense_ref, acc_ref, held, send, recv, own):
    me = coordinates()
    xm, ym, zm, cm = me
    places = (xm * 4 + ym, ym * 4 + zm, xm * 4 + zm)
    third = dense_ref.shape[2] // acc_ref.shape[0]
    greet(me, PLANE_PEERS)
    for k in range(16):
        first, second = k % 4, (k + k // 4) % 4
        for q in range(3):
            offset = ((first, second, 0, 0), (0, first, second, 0), (first, 0, second, 0))[q]
            x, y, z, core = shifted(me, offset)
            place = (x * 4 + y, y * 4 + z, x * 4 + z)[q]
            src = dense_ref.at[q, place]
            dst = held.at[q, places[q]]
            if first == 0 and second == 0:
                pltpu.make_async_copy(src, dst, own.at[q]).start()
            else:
                remote(src, dst, send, recv.at[q], (x, y, z, core)).start()
    for q in range(3):
        pltpu.make_async_copy(dense_ref.at[q, 0], held.at[q, 0], own.at[q]).wait()
        units_wait(held.at[q, 0:15], recv.at[q])

        def one(j, carry):
            start = pl.multiple_of(j * 2 * third, 16)
            total = held[q, 0, pl.ds(start, 2 * third), :].astype(F32)
            for source in range(1, 16):
                total += held[q, source, pl.ds(start, 2 * third), :].astype(F32)
            acc_ref[2 * j, q * third : (q + 1) * third, :] = total[:third]
            acc_ref[2 * j + 1, q * third : (q + 1) * third, :] = total[third:]
            return carry

        lax.fori_loop(0, acc_ref.shape[0] // 2, one, 0)
    units_wait(held.at[:, 0:15], send)


def halves(x):
    high = x.astype(BF16)
    return high, (x - high.astype(F32)).astype(BF16)


def stacked(pairs):
    return jnp.concatenate([part for pair in pairs for part in pair], axis=0)


def products(lefts, right):
    n = right[0].shape[1]
    rows = lefts[0][0].shape[0]
    both = jnp.dot(stacked(lefts), jnp.concatenate(right, axis=1), preferred_element_type=F32)
    found = []
    for k in range(len(lefts)):
        high = both[2 * k * rows : (2 * k + 1) * rows]
        low = both[(2 * k + 1) * rows : (2 * k + 2) * rows]
        found.append(high[:, :n] + (high[:, n:] + low[:, :n]))
    return found


def update_kernel(count, base_ref, acc_ref, pert_ref, mean_ref, out_ref, perts, made, sems, out_sems):
    patches, fields, members, _ = pert_ref.shape

    def take(p):
        return pltpu.make_async_copy(pert_ref.at[p], perts.at[p], sems.at[p])

    def put(p):
        return pltpu.make_async_copy(made.at[p], out_ref.at[p], out_sems.at[p])

    for p in range(patches):
        take(p).start()

    def one(g, carry):
        update_patches(g * count, count, fields, members, base_ref, acc_ref, mean_ref, perts, made, take, put)
        return carry

    lax.fori_loop(0, patches // count, one, 0)
    for p in range(patches):
        put(p).wait()


def update_patches(first, count, fields, members, base_ref, acc_ref, mean_ref, perts, made, take, put):
    half = members // 2
    row = lax.broadcasted_iota(jnp.int32, (members, members), 0)
    lane = lax.broadcasted_iota(jnp.int32, (members, members), 1)
    eye = jnp.where(row == lane, 1.0, 0.0)
    r = row[:half]
    c = lane[:half]
    base = base_ref[0]
    state = []
    for q in range(count):
        packed = acc_ref[first + q, 0:half, :]
        top = jnp.where((c >= half) | (r > c), packed, 0.0)
        low = pltpu.roll(jnp.where((c < half) & (r < c), packed, 0.0), half, 1)
        part = jnp.concatenate([top, low], axis=0)
        own = jnp.sum(jnp.where(r == c, packed, 0.0), axis=0, keepdims=True)
        own = own + pltpu.roll(acc_ref[first + q, half : half + 1, :], half, 1)
        system = part + part.T + jnp.where(row == lane, own + base, 0.0)
        scaling = jnp.sqrt(jnp.sum(jnp.sum(system * system, axis=0, keepdims=True), axis=1, keepdims=True))
        root = system / scaling
        factor = 1.5 * eye - 0.5 * root
        state.append([products([halves(root)], halves(factor))[0], factor, scaling])
    for it in range(1, NS_ITERS):
        for q in range(count):
            root, inverse, _ = state[q]
            root2, inverse2 = halves(root), halves(inverse)
            factor = 1.5 * eye - 0.5 * products([inverse2], root2)[0]
            if it < NS_ITERS - 1:
                state[q][:2] = products([root2, inverse2], halves(factor))
            else:
                state[q][1] = products([inverse2], halves(factor))[0]
    for q in range(count):
        _, inverse, scaling = state[q]
        inverse = inverse * (1.0 / jnp.sqrt(scaling))
        proj = acc_ref[first + q, half + 1 : half + 2, :] + acc_ref[first + q, half + 2 : half + 3, :]
        inverse2 = halves(inverse)
        mean = jnp.broadcast_to(proj, (16, members))
        mean = products([halves(mean)], inverse2)[0]
        mean = products([halves(mean)], inverse2)[0][0:1, :]
        weights = (float(members - 1) ** 0.5 * inverse + mean).astype(BF16)
        take(first + q).wait()
        for f in range(fields):
            change = jnp.dot(weights, perts[first + q, f], preferred_element_type=F32)
            made[first + q, f] = mean_ref[first + q, f : f + 1, :] + change
        put(first + q).start()


def on_device(
    state_pert, state_mean, obs_anom, innov, obs_rinv, obs_lon, obs_lat, block_list, block_count
):
    holders = lax.axis_size(AXES)
    lon_patches, lat_patches, fields, members, columns = state_pert.shape
    patches = lon_patches * lat_patches
    list_length = block_list.shape[2]
    held_blocks, _, block_obs = obs_anom.shape
    slots = patches * list_length
    per = slots // holders
    half = members // 2

    vmem = pl.BlockSpec(memory_space=pltpu.VMEM)
    smem = pl.BlockSpec(memory_space=pltpu.SMEM)
    anywhere = pl.BlockSpec(memory_space=pl.ANY)
    turn = 16
    sums, ext = pl.pallas_call(
        functools.partial(totals_kernel, turn),
        in_specs=[anywhere, vmem, vmem],
        out_specs=[vmem, vmem],
        out_shape=[
            jax.ShapeDtypeStruct((16, block_obs), F32),
            jax.ShapeDtypeStruct((held_blocks, 16, block_obs), BF16),
        ],
        scratch_shapes=[
            pltpu.VMEM((held_blocks, members, block_obs), BF16),
            pltpu.SemaphoreType.DMA((held_blocks // turn,)),
        ],
        name="totals",
    )(obs_anom, obs_rinv, innov)
    first_sum = jnp.sum(sums[0:8])
    second_sum = jnp.sum(sums[8:16]) / (members - 1)

    wanted = block_list.reshape(slots)
    holder = wanted // held_blocks
    slot = jnp.arange(slots)
    patch = slot // list_length
    valid = (slot % list_length < jnp.repeat(block_count.reshape(patches), list_length)).astype(jnp.int32)
    patch_lon, patch_lat = patch // lat_patches, patch % lat_patches
    code = (wanted % held_blocks) * 256 + patch_lat * 128 + patch_lon * PSIDE + valid
    earlier = (holder[:, None] == holder[None, :]) & (slot[None, :] < slot[:, None])
    rank = jnp.sum(earlier.astype(jnp.int32), axis=1)
    bucket = holder * per + rank
    requests = jnp.sum(jnp.where(bucket[:, None] == slot[None, :], code[:, None], 0), axis=0)
    message = jnp.concatenate(
        [
            requests.reshape(holders, per).astype(F32),
            jnp.broadcast_to(jnp.stack([first_sum, second_sum])[None, :], (holders, 2)),
        ],
        axis=1,
    )
    asked = lax.all_to_all(message, AXES, split_axis=0, concat_axis=0, tiled=True)
    total = jnp.sum(asked[:, per:], axis=0)
    inflation = total[0] / (total[1] + holders * held_blocks * block_obs)
    base = ((members - 1) / inflation).reshape(1)
    codes = asked.astype(jnp.int32).reshape(holders * 8)

    third = (half + 8) // 3
    starts = (((codes >> 4) & 7) * lat_patches + ((codes >> 7) & 1)) * third
    got, tables = pl.pallas_call(
        functools.partial(gram_kernel, per, lon_patches, lat_patches),
        in_specs=[pl.BlockSpec(memory_space=pltpu.SMEM), pl.BlockSpec(memory_space=pl.ANY)]
        + [pl.BlockSpec(memory_space=pltpu.VMEM)] * 5,
        out_specs=[pl.BlockSpec(memory_space=pl.ANY)] * 2,
        out_shape=[
            jax.ShapeDtypeStruct((3, 8, 16, per * third, members), BF16),
            jax.ShapeDtypeStruct((3, 8, 8, 128), jnp.int32),
        ],
        scratch_shapes=[
            pltpu.VMEM((holders, 3, per * third, members), BF16),
            pltpu.SemaphoreType.DMA,
            pltpu.SemaphoreType.DMA,
            pltpu.SemaphoreType.DMA,
            pltpu.SemaphoreType.DMA,
            pltpu.SemaphoreType.DMA,
            pltpu.SemaphoreType.DMA((3,)),
        ],
        compiler_params=pltpu.CompilerParams(collective_id=0, has_side_effects=True),
        name="grams",
    )(codes, starts.reshape(8, 128), obs_anom, ext, obs_rinv, obs_lon.astype(F32), obs_lat.astype(F32))

    x, y, z, core = coordinates()
    dense = pl.pallas_call(
        functools.partial(add_kernel, per),
        in_specs=[smem, smem, anywhere],
        out_specs=anywhere,
        out_shape=jax.ShapeDtypeStruct((3, 16, patches * third, members), BF16),
        scratch_shapes=[
            pltpu.VMEM((3, 8, 16, per * third, members), BF16),
            pltpu.VMEM((3, 16, patches * third, members), BF16),
            pltpu.SemaphoreType.DMA((3, 8)),
            pltpu.SemaphoreType.DMA((3,)),
        ]
        + [pltpu.VMEM((patches * third, members), F32)] * CHAINS,
        name="adds",
    )(jnp.stack([x, y, z, core]), tables.reshape(3, 8, 1024), got)

    acc = pl.pallas_call(
        plane_kernel,
        in_specs=[pl.BlockSpec(memory_space=pl.ANY)],
        out_specs=pl.BlockSpec(memory_space=pltpu.VMEM),
        out_shape=jax.ShapeDtypeStruct((patches, half + 8, members), F32),
        scratch_shapes=[
            pltpu.VMEM((3, 16, patches * third, members), BF16),
            pltpu.SemaphoreType.DMA,
            pltpu.SemaphoreType.DMA((3,)),
            pltpu.SemaphoreType.DMA((3,)),
        ],
        compiler_params=pltpu.CompilerParams(collective_id=1, has_side_effects=True),
        name="planes",
    )(dense)

    updated = pl.pallas_call(
        functools.partial(update_kernel, PAIR),
        in_specs=[smem, vmem, anywhere, vmem],
        out_specs=anywhere,
        out_shape=jax.ShapeDtypeStruct((patches, fields, members, columns), F32),
        scratch_shapes=[
            pltpu.VMEM((patches, fields, members, columns), BF16),
            pltpu.VMEM((patches, fields, members, columns), F32),
            pltpu.SemaphoreType.DMA((patches,)),
            pltpu.SemaphoreType.DMA((patches,)),
        ],
        name="update",
    )(
        base,
        acc,
        state_pert.reshape(patches, fields, members, columns),
        state_mean.reshape(patches, fields, columns),
    )
    return updated.reshape(lon_patches, lat_patches, fields, members, columns)


def solution(mesh):
    in_specs = (
        P("lon", "lat", None, None, None),
        P("lon", "lat", None, None),
        P(AXES, None, None),
        P(AXES, None),
        P(AXES, None),
        P(AXES, None),
        P(AXES, None),
        P("lon", "lat", None),
        P("lon", "lat"),
    )
    out_specs = P("lon", "lat", None, None, None)
    return jax.shard_map(
        on_device, mesh=mesh, in_specs=in_specs, out_specs=out_specs, check_vma=False
    )
```

```python
import functools

import jax
import jax.numpy as jnp
from jax import lax
from jax.experimental import pallas as pl
from jax.experimental.pallas import tpu as pltpu
from jax.sharding import PartitionSpec as P

PSIDE = 16
NS_ITERS = 5
LOC_SCALE = 48.0
AXES = ("lon", "lat")
MESH = pl.DeviceIdType.MESH
CHAINS = 2
PAIR = 8
F32 = jnp.float32
BF16 = jnp.bfloat16


def request_kernel(turn, members_less, anom_ref, rinv_ref, innov_ref, ask_ref, got_ref, ext_ref, held, row_out, row_in,
                   sems, send, recv):
    blocks, _, width = anom_ref.shape
    turns = blocks // turn
    holders = ask_ref.shape[0]
    lat_devices = lax.axis_size("lat")
    me = lax.axis_index("lon") * lat_devices + lax.axis_index("lat")

    def copy(k):
        return pltpu.make_async_copy(
            anom_ref.at[pl.ds(k * turn, turn)], held.at[pl.ds(k * turn, turn)], sems.at[k]
        )

    def to_holder(step):
        other = lax.rem(me + step, holders)
        device = (lax.div(other, lat_devices), lax.rem(other, lat_devices))
        return other, device

    for k in range(turns):
        copy(k).start()
    barrier = pltpu.get_barrier_semaphore()

    def signal(step, carry):
        _, device = to_holder(step)
        pl.semaphore_signal(barrier, inc=1, device_id=device, device_id_type=MESH)
        return carry

    lax.fori_loop(1, holders, signal, 0)

    innov = innov_ref[...]
    first = jnp.sum((rinv_ref[...] * innov * innov).reshape(blocks // 8, 8, width), axis=0)

    def one(k, total):
        copy(k).wait()
        start = pl.multiple_of(k * turn, turn)
        rinv = rinv_ref[pl.ds(start, turn), :]
        for b in range(turn):
            a = held[start + b].astype(F32)
            squares = jnp.sum((a * a).reshape(-1, 8, width), axis=0)
            total = total + squares * rinv[b : b + 1, :]
        return total

    second = lax.fori_loop(0, turns, one, jnp.zeros((8, width), F32))

    def whole(x):
        return jnp.sum(jnp.sum(x, axis=0, keepdims=True), axis=1, keepdims=True)

    lane = lax.broadcasted_iota(jnp.int32, (1, width), 1)
    sums = jnp.where(lane == 6, whole(first), 0.0) + jnp.where(lane == 7, whole(second) / members_less, 0.0)
    rows = ask_ref[...] + sums[None]
    row_out[...] = rows
    high = innov.astype(BF16).astype(F32)
    rest = innov - high
    mid = rest.astype(BF16).astype(F32)
    ext = jnp.concatenate(
        [high[:, None, :], mid[:, None, :], (rest - mid)[:, None, :], jnp.zeros((blocks, 13, width), F32)],
        axis=1,
    )
    ext_ref[...] = ext.astype(BF16)
    pl.semaphore_wait(barrier, holders - 1)

    def ask(step, carry):
        other, device = to_holder(step)
        pltpu.make_async_remote_copy(
            src_ref=row_out.at[other],
            dst_ref=row_in.at[me],
            send_sem=send,
            recv_sem=recv,
            device_id=device,
            device_id_type=MESH,
        ).start()
        return carry

    lax.fori_loop(1, holders, ask, 0)
    units_wait(row_out.at[0 : holders - 1], send)
    units_wait(row_in.at[0 : holders - 1], recv)
    got_ref[...] = row_in[...]
    got_ref[me] = row_out[me]


def coordinates():
    lon, lat = lax.axis_index("lon"), lax.axis_index("lat")
    return lax.div(lat, 4), lax.div(lon, 2), lax.rem(lat, 4), lax.rem(lon, 2)


def device_at(x, y, z, core):
    return (y * 2 + core, x * 4 + z)


def units_wait(ref, sem):
    pltpu.make_async_copy(ref, ref, sem).wait()


LINE_PEERS = [(0, 0, 0, 1)] + [
    tuple(step if axis == a else 0 for a in range(3)) + (core,)
    for axis in range(3)
    for step in (1, 2, 3)
    for core in (0, 1)
]
PLANE_PEERS = [
    (dx, dy, dz, 0)
    for dx in range(4)
    for dy in range(4)
    for dz in range(4)
    if 0 < (dx != 0) + (dy != 0) + (dz != 0) < 3
]


def shifted(me, offset):
    x, y, z, core = me
    dx, dy, dz, dc = offset
    return tuple(
        lax.rem(a + d, n) if not isinstance(d, int) or d else a
        for a, d, n in ((x, dx, 4), (y, dy, 4), (z, dz, 4), (core, dc, 2))
    )


def greet(me, offsets):
    barrier = pltpu.get_barrier_semaphore()
    for offset in offsets:
        pl.semaphore_signal(
            barrier, inc=1, device_id=device_at(*shifted(me, offset)), device_id_type=MESH
        )
    pl.semaphore_wait(barrier, len(offsets))


def remote(src, dst, send, recv, target):
    return pltpu.make_async_remote_copy(
        src_ref=src,
        dst_ref=dst,
        send_sem=send,
        recv_sem=recv,
        device_id=device_at(*target),
        device_id_type=MESH,
    )


def gram_kernel(per, lon_patches, lat_patches, code_ref, table_ref, anom_ref, ext_ref, rinv_ref,
                lon_ref, lat_ref, got_ref, codes_ref, stage, send, recv, own, send2, recv2, own2):
    me = coordinates()
    xm, ym, zm, cm = me
    mine = (zm, xm, ym)
    members = anom_ref.shape[1]
    half = members // 2
    third = (half + 8) // 3
    requesters = stage.shape[0]
    grid_lon = float(8 * lon_patches * PSIDE)
    row = lax.broadcasted_iota(jnp.int32, (half, members), 0)
    lane = lax.broadcasted_iota(jnp.int32, (half, members), 1)
    keep = (lane >= half) | (row >= lane)
    on_diag = row == lane
    row8 = lax.broadcasted_iota(jnp.int32, (8, members), 0)

    greet(me, LINE_PEERS)
    for q in range(3):
        source = mine[q] * 2 + cm
        for step in range(4):
            for core in range(2):
                offset = [0, 0, 0, core]
                offset[(2, 0, 1)[q]] = step
                dst = codes_ref.at[q, source]
                if step == 0 and core == 0:
                    pltpu.make_async_copy(table_ref, dst, own2.at[q]).start()
                else:
                    remote(table_ref, dst, send2, recv2, shifted(me, offset)).start()

    def offset_of(i):
        dx = lax.rem(i, 4)
        dy = lax.rem(i + lax.div(i, 4), 4)
        dz = lax.rem(i + lax.div(i, 16), 4)
        return dx, dy, dz, lax.div(i, 64)

    def ship(i):
        dx, dy, dz, dc = offset_of(i)
        x, y, z, core = shifted(me, (dx, dy, dz, dc))
        targets = ((xm, ym, z, core), (x, ym, zm, core), (xm, y, zm, core))
        places = (x * 4 + y, y * 4 + z, x * 4 + z)
        for q, moved in enumerate((dz, dx, dy)):
            src = stage.at[i, q]
            dst = got_ref.at[q, mine[q] * 2 + cm, places[q]]
            stays = (moved == 0) & (dc == 0)

            @pl.when(stays)
            def _():
                pltpu.make_async_copy(src, dst, own).start()

            @pl.when(jnp.logical_not(stays))
            def _():
                remote(src, dst, send, recv, targets[q]).start()

    def one(i, carry):
        x, y, z, core = shifted(me, offset_of(i))
        lon_device = y * 2 + core
        lat_device = x * 4 + z
        who8 = (lon_device * 16 + lat_device) * 8
        lon_first = lon_device * (lon_patches * PSIDE)
        lat_first = lat_device * (lat_patches * PSIDE)
        pieces = []
        for s in range(per):
            code = code_ref[who8 + s]
            valid = code & 1
            held = code >> 8
            cl = (lon_first + (code & 112)).astype(F32) + (PSIDE - 1) / 2.0
            ct = (lat_first + ((code & 128) >> 3)).astype(F32) + (PSIDE - 1) / 2.0
            gap = jnp.abs(lon_ref[pl.ds(held, 1), :].astype(F32) - cl)
            gap = jnp.minimum(gap, grid_lon - gap)
            other = lat_ref[pl.ds(held, 1), :].astype(F32) - ct
            weight = rinv_ref[pl.ds(held, 1), :] * jnp.exp(
                -(gap * gap + other * other) / (2.0 * LOC_SCALE * LOC_SCALE)
            )
            weight = weight * valid.astype(F32)
            a = anom_ref[held]
            scaled = (a.astype(F32) * weight).astype(BF16)
            left = jnp.concatenate([a, ext_ref[held]], axis=0)
            full = lax.dot_general(
                left, scaled, (((1,), (1,)), ((), ())), preferred_element_type=F32
            )
            top = full[:half, :]
            low = pltpu.roll(full[half:members, :], half, 1)
            diag = jnp.sum(jnp.where(on_diag, low, 0.0), axis=0, keepdims=True)
            proj = jnp.sum(full[members : members + 8, :], axis=0, keepdims=True)
            high = proj.astype(BF16).astype(F32)
            extra = jnp.where(
                row8 == 0, diag, jnp.where(row8 == 1, high, jnp.where(row8 == 2, proj - high, 0.0))
            )
            pieces.append(jnp.concatenate([jnp.where(keep, top, low), extra], axis=0))
        for q in range(3):
            for s in range(0, per, 2):
                both = jnp.concatenate(
                    [pieces[s][q * third : (q + 1) * third], pieces[s + 1][q * third : (q + 1) * third]],
                    axis=0,
                )
                stage[i, q, s * third : (s + 2) * third, :] = both.astype(BF16)

        @pl.when(i > 0)
        def _():
            ship(i - 1)

        return carry

    lax.fori_loop(0, requesters, one, 0)
    ship(jnp.int32(requesters - 1))

    for q in range(3):
        pltpu.make_async_copy(table_ref, codes_ref.at[q, 0], own2.at[q]).wait()
    units_wait(codes_ref.at[:, 0:7], send2)
    units_wait(codes_ref.at[:, 0:7], recv2)
    units_wait(stage.at[0:16], own)
    units_wait(stage.at[0:112], send)
    units_wait(got_ref.at[:, 0:7], recv)


def add_kernel(per, me_ref, starts_ref, got_ref, out_ref, held, made, sems, out_sems, *accs):
    sources, places = held.shape[1:3]
    third = held.shape[3] // per
    chains = len(accs)
    row8 = lax.broadcasted_iota(jnp.int32, (8, held.shape[4]), 0)

    def copy(q, source):
        return pltpu.make_async_copy(got_ref.at[q, source], held.at[q, source], sems.at[q, source])

    for q in range(3):
        for source in range(sources):
            copy(q, source).start()
    for q in range(3):
        for source in range(sources):
            copy(q, source).wait()

        def one(place, carry):
            major, minor = lax.div(place, 4), lax.rem(place, 4)
            x = me_ref[0] if q == 1 else major
            y = me_ref[1] if q == 2 else (minor if q == 0 else major)
            z = me_ref[2] if q == 0 else minor
            first = ((y * 2 + me_ref[3]) * 16 + x * 4 + z) * 8
            for acc in accs:
                acc[...] = jnp.zeros_like(acc)
            for source in range(sources):
                for s in range(0, per, 2):
                    both = held[q, source, place, s * third : (s + 2) * third, :].astype(F32)
                    for t in range(2):
                        start = pl.multiple_of(starts_ref[first + ((q * sources + source) * 1024 + s + t)], 8)
                        accs[(s + t) % chains][pl.ds(start, third), :] += both[t * third : (t + 1) * third]
            if q < 2:
                made[q, place] = functools.reduce(lambda a, b: a + b, [acc[...] for acc in accs]).astype(BF16)
            else:
                for p in range(0, accs[0].shape[0] // third, 2):
                    rows = slice(p * third, (p + 2) * third)
                    total = functools.reduce(lambda a, b: a + b, [acc[rows, :] for acc in accs])
                    parts = []
                    for t in range(2):
                        top = total[t * third : t * third + 16]
                        last = total[t * third + 16 : (t + 1) * third]
                        proj = last[1:2, :] + last[2:3, :]
                        high = proj.astype(BF16).astype(F32)
                        parts += [top, jnp.where(row8 == 1, high, jnp.where(row8 == 2, proj - high, last))]
                    made[q, place, rows, :] = jnp.concatenate(parts, axis=0).astype(BF16)
            return carry

        lax.fori_loop(0, places, one, 0)
        pltpu.make_async_copy(made.at[q], out_ref.at[q], out_sems.at[q]).start()
    for q in range(3):
        pltpu.make_async_copy(made.at[q], out_ref.at[q], out_sems.at[q]).wait()


def plane_kernel(dense_ref, acc_ref, held, send, recv, own):
    me = coordinates()
    xm, ym, zm, cm = me
    places = (xm * 4 + ym, ym * 4 + zm, xm * 4 + zm)
    third = dense_ref.shape[2] // acc_ref.shape[0]
    greet(me, PLANE_PEERS)
    for k in range(16):
        first, second = k % 4, (k + k // 4) % 4
        for q in range(3):
            offset = ((first, second, 0, 0), (0, first, second, 0), (first, 0, second, 0))[q]
            x, y, z, core = shifted(me, offset)
            place = (x * 4 + y, y * 4 + z, x * 4 + z)[q]
            src = dense_ref.at[q, place]
            dst = held.at[q, places[q]]
            if first == 0 and second == 0:
                pltpu.make_async_copy(src, dst, own.at[q]).start()
            else:
                remote(src, dst, send, recv.at[q], (x, y, z, core)).start()
    for q in range(3):
        pltpu.make_async_copy(dense_ref.at[q, 0], held.at[q, 0], own.at[q]).wait()
        units_wait(held.at[q, 0:15], recv.at[q])

        def one(j, carry):
            start = pl.multiple_of(j * 2 * third, 16)
            total = held[q, 0, pl.ds(start, 2 * third), :].astype(F32)
            for source in range(1, 16):
                total += held[q, source, pl.ds(start, 2 * third), :].astype(F32)
            acc_ref[2 * j, q * third : (q + 1) * third, :] = total[:third]
            acc_ref[2 * j + 1, q * third : (q + 1) * third, :] = total[third:]
            return carry

        lax.fori_loop(0, acc_ref.shape[0] // 2, one, 0)
    units_wait(held.at[:, 0:15], send)


def halves(x):
    high = x.astype(BF16)
    return high, (x - high.astype(F32)).astype(BF16)


def stacked(pairs):
    return jnp.concatenate([part for pair in pairs for part in pair], axis=0)


def products(lefts, right):
    n = right[0].shape[1]
    rows = lefts[0][0].shape[0]
    both = jnp.dot(stacked(lefts), jnp.concatenate(right, axis=1), preferred_element_type=F32)
    found = []
    for k in range(len(lefts)):
        high = both[2 * k * rows : (2 * k + 1) * rows]
        low = both[(2 * k + 1) * rows : (2 * k + 2) * rows]
        found.append(high[:, :n] + (high[:, n:] + low[:, :n]))
    return found


def update_kernel(count, base_ref, acc_ref, pert_ref, mean_ref, out_ref, perts, made, sems, out_sems):
    patches, fields, members, _ = pert_ref.shape

    def take(p):
        return pltpu.make_async_copy(pert_ref.at[p], perts.at[p], sems.at[p])

    def put(p):
        return pltpu.make_async_copy(made.at[p], out_ref.at[p], out_sems.at[p])

    for p in range(patches):
        take(p).start()

    def one(g, carry):
        update_patches(g * count, count, fields, members, base_ref, acc_ref, mean_ref, perts, made, take, put)
        return carry

    lax.fori_loop(0, patches // count, one, 0)
    for p in range(patches):
        put(p).wait()


def update_patches(first, count, fields, members, base_ref, acc_ref, mean_ref, perts, made, take, put):
    half = members // 2
    row = lax.broadcasted_iota(jnp.int32, (members, members), 0)
    lane = lax.broadcasted_iota(jnp.int32, (members, members), 1)
    eye = jnp.where(row == lane, 1.0, 0.0)
    r = row[:half]
    c = lane[:half]
    base = base_ref[0]
    state = []
    for q in range(count):
        packed = acc_ref[first + q, 0:half, :]
        top = jnp.where((c >= half) | (r > c), packed, 0.0)
        low = pltpu.roll(jnp.where((c < half) & (r < c), packed, 0.0), half, 1)
        part = jnp.concatenate([top, low], axis=0)
        own = jnp.sum(jnp.where(r == c, packed, 0.0), axis=0, keepdims=True)
        own = own + pltpu.roll(acc_ref[first + q, half : half + 1, :], half, 1)
        system = part + part.T + jnp.where(row == lane, own + base, 0.0)
        scaling = jnp.sqrt(jnp.sum(jnp.sum(system * system, axis=0, keepdims=True), axis=1, keepdims=True))
        root = system / scaling
        factor = 1.5 * eye - 0.5 * root
        state.append([products([halves(root)], halves(factor))[0], factor, scaling])
    for it in range(1, NS_ITERS):
        for q in range(count):
            root, inverse, _ = state[q]
            root2, inverse2 = halves(root), halves(inverse)
            factor = 1.5 * eye - 0.5 * products([inverse2], root2)[0]
            if it < NS_ITERS - 1:
                state[q][:2] = products([root2, inverse2], halves(factor))
            else:
                state[q][1] = products([inverse2], halves(factor))[0]
    for q in range(count):
        _, inverse, scaling = state[q]
        inverse = inverse * (1.0 / jnp.sqrt(scaling))
        proj = acc_ref[first + q, half + 1 : half + 2, :] + acc_ref[first + q, half + 2 : half + 3, :]
        inverse2 = halves(inverse)
        mean = jnp.broadcast_to(proj, (16, members))
        mean = products([halves(mean)], inverse2)[0]
        mean = products([halves(mean)], inverse2)[0][0:1, :]
        weights = (float(members - 1) ** 0.5 * inverse + mean).astype(BF16)
        take(first + q).wait()
        for f in range(fields):
            change = jnp.dot(weights, perts[first + q, f], preferred_element_type=F32)
            made[first + q, f] = mean_ref[first + q, f : f + 1, :] + change
        put(first + q).start()


def on_device(
    state_pert, state_mean, obs_anom, innov, obs_rinv, obs_lon, obs_lat, block_list, block_count
):
    holders = lax.axis_size(AXES)
    lon_patches, lat_patches, fields, members, columns = state_pert.shape
    patches = lon_patches * lat_patches
    list_length = block_list.shape[2]
    held_blocks, _, block_obs = obs_anom.shape
    slots = patches * list_length
    per = slots // holders
    half = members // 2

    vmem = pl.BlockSpec(memory_space=pltpu.VMEM)
    smem = pl.BlockSpec(memory_space=pltpu.SMEM)
    anywhere = pl.BlockSpec(memory_space=pl.ANY)
    wanted = block_list.reshape(slots)
    holder = wanted // held_blocks
    slot = jnp.arange(slots)
    patch = slot // list_length
    valid = (slot % list_length < jnp.repeat(block_count.reshape(patches), list_length)).astype(jnp.int32)
    patch_lon, patch_lat = patch // lat_patches, patch % lat_patches
    code = (wanted % held_blocks) * 256 + patch_lat * 128 + patch_lon * PSIDE + valid
    earlier = (holder[:, None] == holder[None, :]) & (slot[None, :] < slot[:, None])
    rank = jnp.sum(earlier.astype(jnp.int32), axis=1)
    bucket = holder * per + rank
    requests = jnp.sum(jnp.where(bucket[:, None] == slot[None, :], code[:, None], 0), axis=0)
    message = jnp.pad(requests.reshape(holders, 1, per).astype(F32), ((0, 0), (0, 0), (0, block_obs - per)))
    turn = 16
    asked, ext = pl.pallas_call(
        functools.partial(request_kernel, turn, float(members - 1)),
        in_specs=[anywhere, vmem, vmem, vmem],
        out_specs=[vmem, vmem],
        out_shape=[
            jax.ShapeDtypeStruct((holders, 1, block_obs), F32),
            jax.ShapeDtypeStruct((held_blocks, 16, block_obs), BF16),
        ],
        scratch_shapes=[
            pltpu.VMEM((held_blocks, members, block_obs), BF16),
            pltpu.VMEM((holders, 1, block_obs), F32),
            pltpu.VMEM((holders, 1, block_obs), F32),
            pltpu.SemaphoreType.DMA((held_blocks // turn,)),
            pltpu.SemaphoreType.DMA,
            pltpu.SemaphoreType.DMA,
        ],
        compiler_params=pltpu.CompilerParams(collective_id=2, has_side_effects=True),
        name="requests",
    )(obs_anom, obs_rinv, innov, message)
    asked = asked.reshape(holders, block_obs)[:, :8]
    total = jnp.sum(asked[:, per:], axis=0)
    inflation = total[0] / (total[1] + holders * held_blocks * block_obs)
    base = ((members - 1) / inflation).reshape(1)
    codes = asked.astype(jnp.int32).reshape(holders * 8)

    third = (half + 8) // 3
    starts = (((codes >> 4) & 7) * lat_patches + ((codes >> 7) & 1)) * third
    got, tables = pl.pallas_call(
        functools.partial(gram_kernel, per, lon_patches, lat_patches),
        in_specs=[pl.BlockSpec(memory_space=pltpu.SMEM), pl.BlockSpec(memory_space=pl.ANY)]
        + [pl.BlockSpec(memory_space=pltpu.VMEM)] * 5,
        out_specs=[pl.BlockSpec(memory_space=pl.ANY)] * 2,
        out_shape=[
            jax.ShapeDtypeStruct((3, 8, 16, per * third, members), BF16),
            jax.ShapeDtypeStruct((3, 8, 8, 128), jnp.int32),
        ],
        scratch_shapes=[
            pltpu.VMEM((holders, 3, per * third, members), BF16),
            pltpu.SemaphoreType.DMA,
            pltpu.SemaphoreType.DMA,
            pltpu.SemaphoreType.DMA,
            pltpu.SemaphoreType.DMA,
            pltpu.SemaphoreType.DMA,
            pltpu.SemaphoreType.DMA((3,)),
        ],
        compiler_params=pltpu.CompilerParams(collective_id=0, has_side_effects=True),
        name="grams",
    )(codes, starts.reshape(8, 128), obs_anom, ext, obs_rinv, obs_lon, obs_lat)

    x, y, z, core = coordinates()
    dense = pl.pallas_call(
        functools.partial(add_kernel, per),
        in_specs=[smem, smem, anywhere],
        out_specs=anywhere,
        out_shape=jax.ShapeDtypeStruct((3, 16, patches * third, members), BF16),
        scratch_shapes=[
            pltpu.VMEM((3, 8, 16, per * third, members), BF16),
            pltpu.VMEM((3, 16, patches * third, members), BF16),
            pltpu.SemaphoreType.DMA((3, 8)),
            pltpu.SemaphoreType.DMA((3,)),
        ]
        + [pltpu.VMEM((patches * third, members), F32)] * CHAINS,
        name="adds",
    )(jnp.stack([x, y, z, core]), tables.reshape(3 * 8 * 1024), got)

    acc = pl.pallas_call(
        plane_kernel,
        in_specs=[pl.BlockSpec(memory_space=pl.ANY)],
        out_specs=pl.BlockSpec(memory_space=pltpu.VMEM),
        out_shape=jax.ShapeDtypeStruct((patches, half + 8, members), F32),
        scratch_shapes=[
            pltpu.VMEM((3, 16, patches * third, members), BF16),
            pltpu.SemaphoreType.DMA,
            pltpu.SemaphoreType.DMA((3,)),
            pltpu.SemaphoreType.DMA((3,)),
        ],
        compiler_params=pltpu.CompilerParams(collective_id=1, has_side_effects=True),
        name="planes",
    )(dense)

    updated = pl.pallas_call(
        functools.partial(update_kernel, PAIR),
        in_specs=[smem, vmem, anywhere, vmem],
        out_specs=anywhere,
        out_shape=jax.ShapeDtypeStruct((patches, fields, members, columns), F32),
        scratch_shapes=[
            pltpu.VMEM((patches, fields, members, columns), BF16),
            pltpu.VMEM((patches, fields, members, columns), F32),
            pltpu.SemaphoreType.DMA((patches,)),
            pltpu.SemaphoreType.DMA((patches,)),
        ],
        name="update",
    )(
        base,
        acc,
        state_pert.reshape(patches, fields, members, columns),
        state_mean.reshape(patches, fields, columns),
    )
    return updated.reshape(lon_patches, lat_patches, fields, members, columns)


def solution(mesh):
    in_specs = (
        P("lon", "lat", None, None, None),
        P("lon", "lat", None, None),
        P(AXES, None, None),
        P(AXES, None),
        P(AXES, None),
        P(AXES, None),
        P(AXES, None),
        P("lon", "lat", None),
        P("lon", "lat"),
    )
    out_specs = P("lon", "lat", None, None, None)
    return jax.shard_map(
        on_device, mesh=mesh, in_specs=in_specs, out_specs=out_specs, check_vma=False
    )
```

```python
import functools

import jax
import jax.numpy as jnp
from jax import lax
from jax.experimental import pallas as pl
from jax.experimental.pallas import tpu as pltpu
from jax.sharding import PartitionSpec as P

PSIDE = 16
NS_ITERS = 5
LOC_SCALE = 48.0
AXES = ("lon", "lat")
MESH = pl.DeviceIdType.MESH
CHAINS = 2
PAIR = 8
F32 = jnp.float32
BF16 = jnp.bfloat16


def request_kernel(turn, members_less, anom_ref, rinv_ref, innov_ref, ask_ref, got_ref, codes_ref, ext_ref, held, row_out, row_in,
                   sems, send, recv):
    blocks, _, width = anom_ref.shape
    turns = blocks // turn
    holders = ask_ref.shape[0]
    lat_devices = lax.axis_size("lat")
    me = lax.axis_index("lon") * lat_devices + lax.axis_index("lat")

    def copy(k):
        return pltpu.make_async_copy(
            anom_ref.at[pl.ds(k * turn, turn)], held.at[pl.ds(k * turn, turn)], sems.at[k]
        )

    def to_holder(step):
        other = lax.rem(me + step, holders)
        device = (lax.div(other, lat_devices), lax.rem(other, lat_devices))
        return other, device

    for k in range(turns):
        copy(k).start()
    barrier = pltpu.get_barrier_semaphore()

    def signal(step, carry):
        _, device = to_holder(step)
        pl.semaphore_signal(barrier, inc=1, device_id=device, device_id_type=MESH)
        return carry

    lax.fori_loop(1, holders, signal, 0)

    innov = innov_ref[...]
    first = jnp.sum((rinv_ref[...] * innov * innov).reshape(blocks // 8, 8, width), axis=0)

    def one(k, total):
        copy(k).wait()
        start = pl.multiple_of(k * turn, turn)
        rinv = rinv_ref[pl.ds(start, turn), :]
        for b in range(turn):
            a = held[start + b].astype(F32)
            squares = jnp.sum((a * a).reshape(-1, 8, width), axis=0)
            total = total + squares * rinv[b : b + 1, :]
        return total

    second = lax.fori_loop(0, turns, one, jnp.zeros((8, width), F32))

    def whole(x):
        return jnp.sum(jnp.sum(x, axis=0, keepdims=True), axis=1, keepdims=True)

    lane = lax.broadcasted_iota(jnp.int32, (1, width), 1)
    sums = jnp.where(lane == 6, whole(first), 0.0) + jnp.where(lane == 7, whole(second) / members_less, 0.0)
    rows = ask_ref[...] + sums[None]
    row_out[...] = rows
    high = innov.astype(BF16).astype(F32)
    rest = innov - high
    mid = rest.astype(BF16).astype(F32)
    ext = jnp.concatenate(
        [high[:, None, :], mid[:, None, :], (rest - mid)[:, None, :], jnp.zeros((blocks, 13, width), F32)],
        axis=1,
    )
    ext_ref[...] = ext.astype(BF16)
    pl.semaphore_wait(barrier, holders - 1)

    def ask(step, carry):
        other, device = to_holder(step)
        pltpu.make_async_remote_copy(
            src_ref=row_out.at[other],
            dst_ref=row_in.at[me],
            send_sem=send,
            recv_sem=recv,
            device_id=device,
            device_id_type=MESH,
        ).start()
        return carry

    lax.fori_loop(1, holders, ask, 0)
    units_wait(row_out.at[0 : holders - 1], send)
    units_wait(row_in.at[0 : holders - 1], recv)
    got_ref[...] = row_in[...]
    got_ref[me] = row_out[me]
    codes_ref[...] = row_in[...].astype(jnp.int32)
    codes_ref[me] = row_out[me].astype(jnp.int32)


def coordinates():
    lon, lat = lax.axis_index("lon"), lax.axis_index("lat")
    return lax.div(lat, 4), lax.div(lon, 2), lax.rem(lat, 4), lax.rem(lon, 2)


def device_at(x, y, z, core):
    return (y * 2 + core, x * 4 + z)


def units_wait(ref, sem):
    pltpu.make_async_copy(ref, ref, sem).wait()


LINE_PEERS = [(0, 0, 0, 1)] + [
    tuple(step if axis == a else 0 for a in range(3)) + (core,)
    for axis in range(3)
    for step in (1, 2, 3)
    for core in (0, 1)
]
AXIS_PEERS = [
    tuple(step if axis == a else 0 for a in range(3)) + (0,) for axis in range(3) for step in (1, 2, 3)
]


def shifted(me, offset):
    x, y, z, core = me
    dx, dy, dz, dc = offset
    return tuple(
        lax.rem(a + d, n) if not isinstance(d, int) or d else a
        for a, d, n in ((x, dx, 4), (y, dy, 4), (z, dz, 4), (core, dc, 2))
    )


def greet(me, offsets):
    barrier = pltpu.get_barrier_semaphore()
    for offset in offsets:
        pl.semaphore_signal(
            barrier, inc=1, device_id=device_at(*shifted(me, offset)), device_id_type=MESH
        )
    pl.semaphore_wait(barrier, len(offsets))


def remote(src, dst, send, recv, target):
    return pltpu.make_async_remote_copy(
        src_ref=src,
        dst_ref=dst,
        send_sem=send,
        recv_sem=recv,
        device_id=device_at(*target),
        device_id_type=MESH,
    )


def gram_kernel(per, lon_patches, lat_patches, code_ref, table_ref, anom_ref, ext_ref, rinv_ref,
                lon_ref, lat_ref, got_ref, codes_ref, stage, blocks, block_sems, send, recv, own, send2, recv2, own2):
    me = coordinates()
    xm, ym, zm, cm = me
    mine = (zm, xm, ym)
    chunks = block_sems.shape[0]
    turn = anom_ref.shape[0] // chunks
    members = anom_ref.shape[1]
    half = members // 2
    third = (half + 8) // 3
    requesters = stage.shape[0]
    grid_lon = float(8 * lon_patches * PSIDE)
    row = lax.broadcasted_iota(jnp.int32, (half, members), 0)
    lane = lax.broadcasted_iota(jnp.int32, (half, members), 1)
    keep = (lane >= half) | (row >= lane)
    on_diag = row == lane
    row8 = lax.broadcasted_iota(jnp.int32, (8, members), 0)

    def fetch(k):
        part = pl.ds(k * turn, turn)
        return pltpu.make_async_copy(anom_ref.at[part], blocks.at[part], block_sems.at[k])

    for k in range(chunks):
        fetch(k).start()
    greet(me, LINE_PEERS)
    for q in range(3):
        source = mine[q] * 2 + cm
        for step in range(4):
            for core in range(2):
                offset = [0, 0, 0, core]
                offset[(2, 0, 1)[q]] = step
                dst = codes_ref.at[q, source]
                if step == 0 and core == 0:
                    pltpu.make_async_copy(table_ref, dst, own2.at[q]).start()
                else:
                    remote(table_ref, dst, send2, recv2, shifted(me, offset)).start()

    for k in range(chunks):
        fetch(k).wait()

    def offset_of(i):
        dx = lax.rem(i, 4)
        dy = lax.rem(i + lax.div(i, 4), 4)
        dz = lax.rem(i + lax.div(i, 16), 4)
        return dx, dy, dz, lax.div(i, 64)

    def ship(i):
        dx, dy, dz, dc = offset_of(i)
        x, y, z, core = shifted(me, (dx, dy, dz, dc))
        targets = ((xm, ym, z, core), (x, ym, zm, core), (xm, y, zm, core))
        places = (x * 4 + y, y * 4 + z, z * 4 + x)
        for q, moved in enumerate((dz, dx, dy)):
            src = stage.at[i, q]
            dst = got_ref.at[q, mine[q] * 2 + cm, places[q]]
            stays = (moved == 0) & (dc == 0)

            @pl.when(stays)
            def _():
                pltpu.make_async_copy(src, dst, own).start()

            @pl.when(jnp.logical_not(stays))
            def _():
                remote(src, dst, send, recv, targets[q]).start()

    def one(i, carry):
        x, y, z, core = shifted(me, offset_of(i))
        lon_device = y * 2 + core
        lat_device = x * 4 + z
        who8 = (lon_device * 16 + lat_device) * members
        lon_first = lon_device * (lon_patches * PSIDE)
        lat_first = lat_device * (lat_patches * PSIDE)
        pieces = []
        for s in range(per):
            code = code_ref[who8 + s]
            valid = code & 1
            held = code >> 8
            cl = (lon_first + (code & 112)).astype(F32) + (PSIDE - 1) / 2.0
            ct = (lat_first + ((code & 128) >> 3)).astype(F32) + (PSIDE - 1) / 2.0
            gap = jnp.abs(lon_ref[pl.ds(held, 1), :].astype(F32) - cl)
            gap = jnp.minimum(gap, grid_lon - gap)
            other = lat_ref[pl.ds(held, 1), :].astype(F32) - ct
            weight = rinv_ref[pl.ds(held, 1), :] * jnp.exp(
                -(gap * gap + other * other) / (2.0 * LOC_SCALE * LOC_SCALE)
            )
            weight = weight * valid.astype(F32)
            a = blocks[held]
            scaled = (a.astype(F32) * weight).astype(BF16)
            left = jnp.concatenate([a, ext_ref[held]], axis=0)
            full = lax.dot_general(
                left, scaled, (((1,), (1,)), ((), ())), preferred_element_type=F32
            )
            top = full[:half, :]
            low = pltpu.roll(full[half:members, :], half, 1)
            diag = jnp.sum(jnp.where(on_diag, low, 0.0), axis=0, keepdims=True)
            proj = jnp.sum(full[members : members + 8, :], axis=0, keepdims=True)
            high = proj.astype(BF16).astype(F32)
            extra = jnp.where(
                row8 == 0, diag, jnp.where(row8 == 1, high, jnp.where(row8 == 2, proj - high, 0.0))
            )
            pieces.append(jnp.concatenate([jnp.where(keep, top, low), extra], axis=0))
        for q in range(3):
            for s in range(0, per, 2):
                both = jnp.concatenate(
                    [pieces[s][q * third : (q + 1) * third], pieces[s + 1][q * third : (q + 1) * third]],
                    axis=0,
                )
                stage[i, q, s * third : (s + 2) * third, :] = both.astype(BF16)

        @pl.when(i > 0)
        def _():
            ship(i - 1)

        return carry

    lax.fori_loop(0, requesters, one, 0)
    ship(jnp.int32(requesters - 1))

    for q in range(3):
        pltpu.make_async_copy(table_ref, codes_ref.at[q, 0], own2.at[q]).wait()
    units_wait(codes_ref.at[:, 0:7], send2)
    units_wait(codes_ref.at[:, 0:7], recv2)
    units_wait(stage.at[0:16], own)
    units_wait(stage.at[0:112], send)
    units_wait(got_ref.at[:, 0:7], recv)


def split_again(total, third):
    row8 = lax.broadcasted_iota(jnp.int32, (8, total.shape[1]), 0)
    parts = []
    for t in range(2):
        top = total[t * third : t * third + 16]
        last = total[t * third + 16 : (t + 1) * third]
        proj = last[1:2, :] + last[2:3, :]
        high = proj.astype(BF16).astype(F32)
        parts += [top, jnp.where(row8 == 1, high, jnp.where(row8 == 2, proj - high, last))]
    return jnp.concatenate(parts, axis=0)


def add_kernel(per, starts_ref, got_ref, out_ref, held, made, sems, out_sems, *accs):
    sources, places = held.shape[1:3]
    third = held.shape[3] // per
    chains = len(accs)
    xm, ym, zm, cm = coordinates()

    def copy(q, source):
        return pltpu.make_async_copy(got_ref.at[q, source], held.at[q, source], sems.at[q, source])

    for q in range(3):
        for source in range(sources):
            copy(q, source).start()
    for q in range(3):
        for source in range(sources):
            copy(q, source).wait()

        def one(place, carry):
            major, minor = lax.div(place, 4), lax.rem(place, 4)
            x = (major, xm, minor)[q]
            y = (minor, major, ym)[q]
            z = (zm, minor, major)[q]
            first = ((y * 2 + cm) * 16 + x * 4 + z) * 8
            for acc in accs:
                acc[...] = jnp.zeros_like(acc)
            for source in range(sources):
                for s in range(0, per, 2):
                    both = held[q, source, place, s * third : (s + 2) * third, :].astype(F32)
                    for t in range(2):
                        start = pl.multiple_of(starts_ref[first + ((q * sources + source) * 1024 + s + t)], 8)
                        accs[(s + t) % chains][pl.ds(start, third), :] += both[t * third : (t + 1) * third]
            if q < 2:
                made[q, place] = functools.reduce(lambda a, b: a + b, [acc[...] for acc in accs]).astype(BF16)
            else:
                for p in range(0, accs[0].shape[0] // third, 2):
                    rows = slice(p * third, (p + 2) * third)
                    total = functools.reduce(lambda a, b: a + b, [acc[rows, :] for acc in accs])
                    made[q, place, rows, :] = split_again(total, third).astype(BF16)
            return carry

        lax.fori_loop(0, places, one, 0)
        pltpu.make_async_copy(made.at[q], out_ref.at[q], out_sems.at[q]).start()
    for q in range(3):
        pltpu.make_async_copy(made.at[q], out_ref.at[q], out_sems.at[q]).wait()


def plane_kernel(dense_ref, acc_ref, held, mids, lasts, send, recv, send2, recv2, own):
    me = coordinates()
    xm, ym, zm, _ = me
    firsts, seconds = (xm, ym, zm), (ym, zm, xm)
    rows = dense_ref.shape[2]
    third = rows // acc_ref.shape[0]

    def along(axis, step):
        return shifted(me, tuple(step if a == axis else 0 for a in range(3)) + (0,))

    greet(me, AXIS_PEERS)
    for q in range(3):
        mine = dense_ref.at[q, pl.ds(firsts[q] * 4, 4)]
        pltpu.make_async_copy(mine, held.at[q, firsts[q]], own.at[q]).start()
    for step in (2, 1, 3):
        for q in range(3):
            other = lax.rem(firsts[q] + step, 4)
            remote(
                dense_ref.at[q, pl.ds(other * 4, 4)], held.at[q, firsts[q]], send, recv.at[q],
                along(q, step),
            ).start()
    for q in range(3):
        pltpu.make_async_copy(dense_ref.at[q, 0:4], held.at[q, 0], own.at[q]).wait()
        units_wait(held.at[q, 0:3], recv.at[q])

        def one(k, carry):
            place = lax.rem(seconds[q] + 1 + lax.div(k, rows // (2 * third)), 4)
            start = pl.multiple_of(lax.rem(k, rows // (2 * third)) * (2 * third), 16)
            total = held[q, 0, place, pl.ds(start, 2 * third), :].astype(F32)
            for source in range(1, 4):
                total += held[q, source, place, pl.ds(start, 2 * third), :].astype(F32)
            if q == 2:
                total = split_again(total, third)
            mids[q, place, pl.ds(start, 2 * third), :] = total.astype(BF16)
            return carry

        lax.fori_loop(0, 4 * rows // (2 * third), one, 0)
        for step in (2, 1, 3):
            other = lax.rem(seconds[q] + step, 4)
            remote(
                mids.at[q, other], lasts.at[q, seconds[q]], send2, recv2.at[q], along((q + 1) % 3, step)
            ).start()
        lasts[q, seconds[q]] = mids[q, seconds[q]]
    for q in range(3):
        units_wait(lasts.at[q, 0:3], recv2.at[q])

        def two(j, carry):
            start = pl.multiple_of(j * 2 * third, 16)
            total = lasts[q, 0, pl.ds(start, 2 * third), :].astype(F32)
            for source in range(1, 4):
                total += lasts[q, source, pl.ds(start, 2 * third), :].astype(F32)
            acc_ref[2 * j, q * third : (q + 1) * third, :] = total[:third]
            acc_ref[2 * j + 1, q * third : (q + 1) * third, :] = total[third:]
            return carry

        lax.fori_loop(0, acc_ref.shape[0] // 2, two, 0)
    units_wait(held.at[:, 0:3], send)
    units_wait(lasts.at[:, 0:3], send2)


def halves(x):
    high = x.astype(BF16)
    return high, (x - high.astype(F32)).astype(BF16)


def stacked(pairs):
    return jnp.concatenate([part for pair in pairs for part in pair], axis=0)


def products(lefts, right):
    n = right[0].shape[1]
    rows = lefts[0][0].shape[0]
    both = jnp.dot(stacked(lefts), jnp.concatenate(right, axis=1), preferred_element_type=F32)
    found = []
    for k in range(len(lefts)):
        high = both[2 * k * rows : (2 * k + 1) * rows]
        low = both[(2 * k + 1) * rows : (2 * k + 2) * rows]
        found.append(high[:, :n] + (high[:, n:] + low[:, :n]))
    return found


def update_kernel(count, observations, asked_ref, acc_ref, pert_ref, mean_ref, out_ref, perts, made, sems, out_sems):
    patches, fields, members, _ = pert_ref.shape

    def take(p):
        return pltpu.make_async_copy(pert_ref.at[p], perts.at[p], sems.at[p])

    def put(p):
        return pltpu.make_async_copy(made.at[p], out_ref.at[p], out_sems.at[p])

    for p in range(patches):
        take(p).start()
    base = float(members - 1) / base_of(asked_ref, observations)

    def one(g, carry):
        update_patches(g * count, count, fields, members, base, acc_ref, mean_ref, perts, made, take, put)
        return carry

    lax.fori_loop(0, patches // count, one, 0)
    for p in range(patches):
        put(p).wait()


def base_of(asked_ref, observations):
    total = jnp.sum(asked_ref[...], axis=0)
    lane = lax.broadcasted_iota(jnp.int32, total.shape, 1)
    first = jnp.sum(jnp.where(lane == 6, total, 0.0), axis=1, keepdims=True)
    second = jnp.sum(jnp.where(lane == 7, total, 0.0), axis=1, keepdims=True)
    return first / (second + float(observations))


def update_patches(first, count, fields, members, base, acc_ref, mean_ref, perts, made, take, put):
    half = members // 2
    row = lax.broadcasted_iota(jnp.int32, (members, members), 0)
    lane = lax.broadcasted_iota(jnp.int32, (members, members), 1)
    eye = jnp.where(row == lane, 1.0, 0.0)
    r = row[:half]
    c = lane[:half]
    state = []
    for q in range(count):
        packed = acc_ref[first + q, 0:half, :]
        top = jnp.where((c >= half) | (r > c), packed, 0.0)
        low = pltpu.roll(jnp.where((c < half) & (r < c), packed, 0.0), half, 1)
        part = jnp.concatenate([top, low], axis=0)
        own = jnp.sum(jnp.where(r == c, packed, 0.0), axis=0, keepdims=True)
        own = own + pltpu.roll(acc_ref[first + q, half : half + 1, :], half, 1)
        system = part + part.T + jnp.where(row == lane, own + base, 0.0)
        scaling = jnp.sqrt(jnp.sum(jnp.sum(system * system, axis=0, keepdims=True), axis=1, keepdims=True))
        root = system / scaling
        factor = 1.5 * eye - 0.5 * root
        state.append([products([halves(root)], halves(factor))[0], factor, scaling])
    for it in range(1, NS_ITERS):
        for q in range(count):
            root, inverse, _ = state[q]
            root2, inverse2 = halves(root), halves(inverse)
            factor = 1.5 * eye - 0.5 * products([inverse2], root2)[0]
            if it < NS_ITERS - 1:
                state[q][:2] = products([root2, inverse2], halves(factor))
            else:
                state[q][1] = products([inverse2], halves(factor))[0]
    for q in range(count):
        _, inverse, scaling = state[q]
        inverse = inverse * (1.0 / jnp.sqrt(scaling))
        proj = acc_ref[first + q, half + 1 : half + 2, :] + acc_ref[first + q, half + 2 : half + 3, :]
        inverse2 = halves(inverse)
        mean = jnp.broadcast_to(proj, (16, members))
        mean = products([halves(mean)], inverse2)[0]
        mean = products([halves(mean)], inverse2)[0][0:1, :]
        weights = (float(members - 1) ** 0.5 * inverse + mean).astype(BF16)
        take(first + q).wait()
        for f in range(fields):
            change = jnp.dot(weights, perts[first + q, f], preferred_element_type=F32)
            made[first + q, f] = mean_ref[first + q, f : f + 1, :] + change
        put(first + q).start()


def on_device(
    state_pert, state_mean, obs_anom, innov, obs_rinv, obs_lon, obs_lat, block_list, block_count
):
    holders = lax.axis_size(AXES)
    lon_patches, lat_patches, fields, members, columns = state_pert.shape
    patches = lon_patches * lat_patches
    list_length = block_list.shape[2]
    held_blocks, _, block_obs = obs_anom.shape
    slots = patches * list_length
    per = slots // holders
    half = members // 2

    vmem = pl.BlockSpec(memory_space=pltpu.VMEM)
    smem = pl.BlockSpec(memory_space=pltpu.SMEM)
    anywhere = pl.BlockSpec(memory_space=pl.ANY)
    wanted = block_list.reshape(slots)
    holder = wanted // held_blocks
    slot = jnp.arange(slots)
    patch = slot // list_length
    valid = (slot % list_length < jnp.repeat(block_count.reshape(patches), list_length)).astype(jnp.int32)
    patch_lon, patch_lat = patch // lat_patches, patch % lat_patches
    code = (wanted % held_blocks) * 256 + patch_lat * 128 + patch_lon * PSIDE + valid
    earlier = (holder[:, None] == holder[None, :]) & (slot[None, :] < slot[:, None])
    rank = jnp.sum(earlier.astype(jnp.int32), axis=1)
    bucket = holder * per + rank
    requests = jnp.sum(jnp.where(bucket[:, None] == slot[None, :], code[:, None], 0), axis=0)
    message = jnp.pad(requests.reshape(holders, 1, per).astype(F32), ((0, 0), (0, 0), (0, block_obs - per)))
    turn = 16
    asked, codes, ext = pl.pallas_call(
        functools.partial(request_kernel, turn, float(members - 1)),
        in_specs=[anywhere, vmem, vmem, vmem],
        out_specs=[vmem, vmem, vmem],
        out_shape=[
            jax.ShapeDtypeStruct((holders, 1, block_obs), F32),
            jax.ShapeDtypeStruct((holders, 1, block_obs), jnp.int32),
            jax.ShapeDtypeStruct((held_blocks, 16, block_obs), BF16),
        ],
        scratch_shapes=[
            pltpu.VMEM((held_blocks, members, block_obs), BF16),
            pltpu.VMEM((holders, 1, block_obs), F32),
            pltpu.VMEM((holders, 1, block_obs), F32),
            pltpu.SemaphoreType.DMA((held_blocks // turn,)),
            pltpu.SemaphoreType.DMA,
            pltpu.SemaphoreType.DMA,
        ],
        compiler_params=pltpu.CompilerParams(collective_id=2, has_side_effects=True),
        name="requests",
    )(obs_anom, obs_rinv, innov, message)
    third = (half + 8) // 3
    short = codes.reshape(holders, block_obs)[:, :8].reshape(holders * 8)
    starts = (((short >> 4) & 7) * lat_patches + ((short >> 7) & 1)) * third
    got, tables = pl.pallas_call(
        functools.partial(gram_kernel, per, lon_patches, lat_patches),
        in_specs=[smem, anywhere, anywhere, vmem, vmem, vmem, vmem],
        out_specs=[pl.BlockSpec(memory_space=pl.ANY)] * 2,
        out_shape=[
            jax.ShapeDtypeStruct((3, 8, 16, per * third, members), BF16),
            jax.ShapeDtypeStruct((3, 8, 8, 128), jnp.int32),
        ],
        scratch_shapes=[
            pltpu.VMEM((holders, 3, per * third, members), BF16),
            pltpu.VMEM((held_blocks, members, block_obs), BF16),
            pltpu.SemaphoreType.DMA((held_blocks // turn,)),
            pltpu.SemaphoreType.DMA,
            pltpu.SemaphoreType.DMA,
            pltpu.SemaphoreType.DMA,
            pltpu.SemaphoreType.DMA,
            pltpu.SemaphoreType.DMA,
            pltpu.SemaphoreType.DMA((3,)),
        ],
        compiler_params=pltpu.CompilerParams(collective_id=0, has_side_effects=True),
        name="grams",
    )(codes.reshape(holders * block_obs), starts.reshape(8, 128), obs_anom, ext, obs_rinv, obs_lon, obs_lat)

    dense = pl.pallas_call(
        functools.partial(add_kernel, per),
        in_specs=[smem, anywhere],
        out_specs=anywhere,
        out_shape=jax.ShapeDtypeStruct((3, 16, patches * third, members), BF16),
        scratch_shapes=[
            pltpu.VMEM((3, 8, 16, per * third, members), BF16),
            pltpu.VMEM((3, 16, patches * third, members), BF16),
            pltpu.SemaphoreType.DMA((3, 8)),
            pltpu.SemaphoreType.DMA((3,)),
        ]
        + [pltpu.VMEM((patches * third, members), F32)] * CHAINS,
        name="adds",
    )(tables.reshape(3 * 8 * 1024), got)

    acc = pl.pallas_call(
        plane_kernel,
        in_specs=[pl.BlockSpec(memory_space=pl.ANY)],
        out_specs=pl.BlockSpec(memory_space=pltpu.VMEM),
        out_shape=jax.ShapeDtypeStruct((patches, half + 8, members), F32),
        scratch_shapes=[
            pltpu.VMEM((3, 4, 4, patches * third, members), BF16),
            pltpu.VMEM((3, 4, patches * third, members), BF16),
            pltpu.VMEM((3, 4, patches * third, members), BF16),
            pltpu.SemaphoreType.DMA,
            pltpu.SemaphoreType.DMA((3,)),
            pltpu.SemaphoreType.DMA,
            pltpu.SemaphoreType.DMA((3,)),
            pltpu.SemaphoreType.DMA((3,)),
        ],
        compiler_params=pltpu.CompilerParams(collective_id=1, has_side_effects=True),
        name="planes",
    )(dense)

    updated = pl.pallas_call(
        functools.partial(update_kernel, PAIR, holders * held_blocks * block_obs),
        in_specs=[vmem, vmem, anywhere, vmem],
        out_specs=anywhere,
        out_shape=jax.ShapeDtypeStruct((patches, fields, members, columns), F32),
        scratch_shapes=[
            pltpu.VMEM((patches, fields, members, columns), BF16),
            pltpu.VMEM((patches, fields, members, columns), F32),
            pltpu.SemaphoreType.DMA((patches,)),
            pltpu.SemaphoreType.DMA((patches,)),
        ],
        name="update",
    )(
        asked,
        acc,
        state_pert.reshape(patches, fields, members, columns),
        state_mean.reshape(patches, fields, columns),
    )
    return updated.reshape(lon_patches, lat_patches, fields, members, columns)


def solution(mesh):
    in_specs = (
        P("lon", "lat", None, None, None),
        P("lon", "lat", None, None),
        P(AXES, None, None),
        P(AXES, None),
        P(AXES, None),
        P(AXES, None),
        P(AXES, None),
        P("lon", "lat", None),
        P("lon", "lat"),
    )
    out_specs = P("lon", "lat", None, None, None)
    return jax.shard_map(
        on_device, mesh=mesh, in_specs=in_specs, out_specs=out_specs, check_vma=False
    )
```

```python
import functools

import jax
import jax.numpy as jnp
from jax import lax
from jax.experimental import pallas as pl
from jax.experimental.pallas import tpu as pltpu
from jax.sharding import PartitionSpec as P

PSIDE = 16
NS_ITERS = 5
LOC_SCALE = 48.0
AXES = ("lon", "lat")
MESH = pl.DeviceIdType.MESH
CHAINS = 2
PAIR = 8
F32 = jnp.float32
BF16 = jnp.bfloat16


def request_kernel(turn, members_less, anom_ref, rinv_ref, innov_ref, ask_ref, codes_ref, sums_ref, ext_ref, held,
                   row_in, sems, send, recv):
    blocks, _, width = anom_ref.shape
    turns = blocks // turn
    holders = ask_ref.shape[0]
    lat_devices = lax.axis_size("lat")
    me = lax.axis_index("lon") * lat_devices + lax.axis_index("lat")

    def copy(k):
        return pltpu.make_async_copy(
            anom_ref.at[pl.ds(k * turn, turn)], held.at[pl.ds(k * turn, turn)], sems.at[k]
        )

    def to_holder(step):
        other = lax.rem(me + step, holders)
        device = (lax.div(other, lat_devices), lax.rem(other, lat_devices))
        return other, device

    barrier = pltpu.get_barrier_semaphore()

    def signal(step, carry):
        _, device = to_holder(step)
        pl.semaphore_signal(barrier, inc=1, device_id=device, device_id_type=MESH)
        return carry

    lax.fori_loop(1, holders, signal, 0)
    for k in range(turns):
        copy(k).start()
    innov = innov_ref[...]
    high = innov.astype(BF16).astype(F32)
    rest = innov - high
    mid = rest.astype(BF16).astype(F32)
    ext = jnp.concatenate(
        [high[:, None, :], mid[:, None, :], (rest - mid)[:, None, :], jnp.zeros((blocks, 13, width), F32)],
        axis=1,
    )
    ext_ref[...] = ext.astype(BF16)
    first = jnp.sum((rinv_ref[...] * innov * innov).reshape(blocks // 8, 8, width), axis=0)
    pl.semaphore_wait(barrier, holders - 1)

    def ask(step, carry):
        other, device = to_holder(step)
        pltpu.make_async_remote_copy(
            src_ref=ask_ref.at[other],
            dst_ref=row_in.at[me],
            send_sem=send,
            recv_sem=recv,
            device_id=device,
            device_id_type=MESH,
        ).start()
        return carry

    lax.fori_loop(1, holders, ask, 0)

    def one(k, total):
        copy(k).wait()
        start = pl.multiple_of(k * turn, turn)
        rinv = rinv_ref[pl.ds(start, turn), :]
        for b in range(turn):
            a = held[start + b].astype(F32)
            squares = jnp.sum((a * a).reshape(-1, 8, width), axis=0)
            total = total + squares * rinv[b : b + 1, :]
        return total

    second = lax.fori_loop(0, turns, one, jnp.zeros((8, width), F32))

    def whole(x):
        return jnp.sum(jnp.sum(x, axis=0, keepdims=True), axis=1, keepdims=True)

    lane = lax.broadcasted_iota(jnp.int32, (8, width), 1)
    sums_ref[...] = jnp.where(
        lane == 0, whole(first), jnp.where(lane == 1, whole(second) / members_less, 0.0)
    )
    units_wait(row_in.at[0 : holders - 1], send)
    units_wait(row_in.at[0 : holders - 1], recv)
    codes_ref[...] = row_in[...]
    codes_ref[me] = ask_ref[me]


def coordinates():
    lon, lat = lax.axis_index("lon"), lax.axis_index("lat")
    return lax.div(lat, 4), lax.div(lon, 2), lax.rem(lat, 4), lax.rem(lon, 2)


def device_at(x, y, z, core):
    return (y * 2 + core, x * 4 + z)


def units_wait(ref, sem):
    pltpu.make_async_copy(ref, ref, sem).wait()


LINE_PEERS = [(0, 0, 0, 1)] + [
    tuple(step if axis == a else 0 for a in range(3)) + (core,)
    for axis in range(3)
    for step in (1, 2, 3)
    for core in (0, 1)
]
AXIS_PEERS = [
    tuple(step if axis == a else 0 for a in range(3)) + (0,) for axis in range(3) for step in (1, 2, 3)
]


def shifted(me, offset):
    x, y, z, core = me
    dx, dy, dz, dc = offset
    return tuple(
        lax.rem(a + d, n) if not isinstance(d, int) or d else a
        for a, d, n in ((x, dx, 4), (y, dy, 4), (z, dz, 4), (core, dc, 2))
    )


def greet(me, offsets):
    barrier = pltpu.get_barrier_semaphore()
    for offset in offsets:
        pl.semaphore_signal(
            barrier, inc=1, device_id=device_at(*shifted(me, offset)), device_id_type=MESH
        )
    pl.semaphore_wait(barrier, len(offsets))


def remote(src, dst, send, recv, target):
    return pltpu.make_async_remote_copy(
        src_ref=src,
        dst_ref=dst,
        send_sem=send,
        recv_sem=recv,
        device_id=device_at(*target),
        device_id_type=MESH,
    )


def gram_kernel(per, lon_patches, lat_patches, code_ref, table_ref, sums_ref, anom_ref, ext_ref, rinv_ref,
                lon_ref, lat_ref, got_ref, codes_ref, lines_ref, stage, blocks, block_sems, send, recv, own,
                send2, recv2, own2, send3, recv3, own3):
    me = coordinates()
    xm, ym, zm, cm = me
    mine = (zm, xm, ym)
    chunks = block_sems.shape[0]
    turn = anom_ref.shape[0] // chunks
    members = anom_ref.shape[1]
    half = members // 2
    third = (half + 8) // 3
    requesters = stage.shape[0]
    grid_lon = float(8 * lon_patches * PSIDE)
    row = lax.broadcasted_iota(jnp.int32, (half, members), 0)
    lane = lax.broadcasted_iota(jnp.int32, (half, members), 1)
    keep = (lane >= half) | (row >= lane)
    on_diag = row == lane
    row8 = lax.broadcasted_iota(jnp.int32, (8, members), 0)

    def fetch(k):
        part = pl.ds(k * turn, turn)
        return pltpu.make_async_copy(anom_ref.at[part], blocks.at[part], block_sems.at[k])

    for k in range(chunks):
        fetch(k).start()
    greet(me, LINE_PEERS)
    for q in range(3):
        source = mine[q] * 2 + cm
        for step in range(4):
            for core in range(2):
                offset = [0, 0, 0, core]
                offset[(2, 0, 1)[q]] = step
                dst = codes_ref.at[q, source]
                if step == 0 and core == 0:
                    pltpu.make_async_copy(table_ref, dst, own2.at[q]).start()
                else:
                    remote(table_ref, dst, send2, recv2, shifted(me, offset)).start()
                if q == 0:
                    line = lines_ref.at[source]
                    if step == 0 and core == 0:
                        pltpu.make_async_copy(sums_ref, line, own3).start()
                    else:
                        remote(sums_ref, line, send3, recv3, shifted(me, offset)).start()

    for k in range(chunks):
        fetch(k).wait()

    def offset_of(i):
        dx = lax.rem(i, 4)
        dy = lax.rem(i + lax.div(i, 4), 4)
        dz = lax.rem(i + lax.div(i, 16), 4)
        return dx, dy, dz, lax.div(i, 64)

    def ship(i):
        dx, dy, dz, dc = offset_of(i)
        x, y, z, core = shifted(me, (dx, dy, dz, dc))
        targets = ((xm, ym, z, core), (x, ym, zm, core), (xm, y, zm, core))
        places = (x * 4 + y, y * 4 + z, z * 4 + x)
        for q, moved in enumerate((dz, dx, dy)):
            src = stage.at[i, q]
            dst = got_ref.at[q, mine[q] * 2 + cm, places[q]]
            stays = (moved == 0) & (dc == 0)

            @pl.when(stays)
            def _():
                pltpu.make_async_copy(src, dst, own).start()

            @pl.when(jnp.logical_not(stays))
            def _():
                remote(src, dst, send, recv, targets[q]).start()

    def one(i, carry):
        x, y, z, core = shifted(me, offset_of(i))
        lon_device = y * 2 + core
        lat_device = x * 4 + z
        who8 = (lon_device * 16 + lat_device) * members
        lon_first = lon_device * (lon_patches * PSIDE)
        lat_first = lat_device * (lat_patches * PSIDE)
        pieces = []
        for s in range(per):
            code = code_ref[who8 + s]
            valid = code & 1
            held = code >> 8
            cl = (lon_first + (code & 112)).astype(F32) + (PSIDE - 1) / 2.0
            ct = (lat_first + ((code & 128) >> 3)).astype(F32) + (PSIDE - 1) / 2.0
            gap = jnp.abs(lon_ref[pl.ds(held, 1), :].astype(F32) - cl)
            gap = jnp.minimum(gap, grid_lon - gap)
            other = lat_ref[pl.ds(held, 1), :].astype(F32) - ct
            weight = rinv_ref[pl.ds(held, 1), :] * jnp.exp(
                -(gap * gap + other * other) / (2.0 * LOC_SCALE * LOC_SCALE)
            )
            weight = weight * valid.astype(F32)
            a = blocks[held]
            scaled = (a.astype(F32) * weight).astype(BF16)
            left = jnp.concatenate([a, ext_ref[held]], axis=0)
            full = lax.dot_general(
                left, scaled, (((1,), (1,)), ((), ())), preferred_element_type=F32
            )
            top = full[:half, :]
            low = pltpu.roll(full[half:members, :], half, 1)
            diag = jnp.sum(jnp.where(on_diag, low, 0.0), axis=0, keepdims=True)
            proj = jnp.sum(full[members : members + 8, :], axis=0, keepdims=True)
            high = proj.astype(BF16).astype(F32)
            extra = jnp.where(
                row8 == 0, diag, jnp.where(row8 == 1, high, jnp.where(row8 == 2, proj - high, 0.0))
            )
            pieces.append(jnp.concatenate([jnp.where(keep, top, low), extra], axis=0))
        for q in range(3):
            for s in range(0, per, 2):
                both = jnp.concatenate(
                    [pieces[s][q * third : (q + 1) * third], pieces[s + 1][q * third : (q + 1) * third]],
                    axis=0,
                )
                stage[i, q, s * third : (s + 2) * third, :] = both.astype(BF16)

        @pl.when(i > 0)
        def _():
            ship(i - 1)

        return carry

    lax.fori_loop(0, requesters, one, 0)
    ship(jnp.int32(requesters - 1))

    for q in range(3):
        pltpu.make_async_copy(table_ref, codes_ref.at[q, 0], own2.at[q]).wait()
    pltpu.make_async_copy(sums_ref, lines_ref.at[0], own3).wait()
    units_wait(lines_ref.at[0:7], send3)
    units_wait(lines_ref.at[0:7], recv3)
    units_wait(codes_ref.at[:, 0:7], send2)
    units_wait(codes_ref.at[:, 0:7], recv2)
    units_wait(stage.at[0:16], own)
    units_wait(stage.at[0:112], send)
    units_wait(got_ref.at[:, 0:7], recv)


def split_again(total, third):
    row8 = lax.broadcasted_iota(jnp.int32, (8, total.shape[1]), 0)
    parts = []
    for t in range(2):
        top = total[t * third : t * third + 16]
        last = total[t * third + 16 : (t + 1) * third]
        proj = last[1:2, :] + last[2:3, :]
        high = proj.astype(BF16).astype(F32)
        parts += [top, jnp.where(row8 == 1, high, jnp.where(row8 == 2, proj - high, last))]
    return jnp.concatenate(parts, axis=0)


def add_kernel(per, starts_ref, got_ref, out_ref, held, made, sems, out_sems, *accs):
    sources, places = held.shape[1:3]
    third = held.shape[3] // per
    chains = len(accs)
    xm, ym, zm, cm = coordinates()

    def copy(q, source):
        return pltpu.make_async_copy(got_ref.at[q, source], held.at[q, source], sems.at[q, source])

    for q in range(3):
        for source in range(sources):
            copy(q, source).start()
    for q in range(3):
        for source in range(sources):
            copy(q, source).wait()

        def one(place, carry):
            major, minor = lax.div(place, 4), lax.rem(place, 4)
            x = (major, xm, minor)[q]
            y = (minor, major, ym)[q]
            z = (zm, minor, major)[q]
            first = ((y * 2 + cm) * 16 + x * 4 + z) * 8
            for acc in accs:
                acc[...] = jnp.zeros_like(acc)
            for source in range(sources):
                for s in range(0, per, 2):
                    both = held[q, source, place, s * third : (s + 2) * third, :].astype(F32)
                    for t in range(2):
                        start = pl.multiple_of(starts_ref[first + ((q * sources + source) * 1024 + s + t)], 8)
                        accs[(s + t) % chains][pl.ds(start, third), :] += both[t * third : (t + 1) * third]
            if q < 2:
                made[q, place] = functools.reduce(lambda a, b: a + b, [acc[...] for acc in accs]).astype(BF16)
            else:
                for p in range(0, accs[0].shape[0] // third, 2):
                    rows = slice(p * third, (p + 2) * third)
                    total = functools.reduce(lambda a, b: a + b, [acc[rows, :] for acc in accs])
                    made[q, place, rows, :] = split_again(total, third).astype(BF16)
            return carry

        lax.fori_loop(0, places, one, 0)
        pltpu.make_async_copy(made.at[q], out_ref.at[q], out_sems.at[q]).start()
    for q in range(3):
        pltpu.make_async_copy(made.at[q], out_ref.at[q], out_sems.at[q]).wait()


def plane_kernel(dense_ref, lines_ref, acc_ref, total_ref, held, mids, lasts, sums, parts, send, recv, send2, recv2,
                 own, send3, recv3):
    me = coordinates()
    xm, ym, zm, _ = me
    firsts, seconds = (xm, ym, zm), (ym, zm, xm)
    rows = dense_ref.shape[2]
    third = rows // acc_ref.shape[0]

    def along(axis, step):
        return shifted(me, tuple(step if a == axis else 0 for a in range(3)) + (0,))

    def give_sums(axis):
        here = (xm, ym)[axis]
        for step in (2, 1, 3):
            remote(sums.at[axis], parts.at[axis, here], send3.at[axis], recv3.at[axis], along(axis, step)).start()
        parts[axis, here] = sums[axis]

    def take_sums(axis):
        units_wait(parts.at[axis, 0:3], send3.at[axis])
        units_wait(parts.at[axis, 0:3], recv3.at[axis])
        return jnp.sum(parts[axis], axis=0)

    sums[0] = jnp.sum(lines_ref[...], axis=0)
    greet(me, AXIS_PEERS)
    give_sums(0)
    for q in range(3):
        mine = dense_ref.at[q, pl.ds(firsts[q] * 4, 4)]
        pltpu.make_async_copy(mine, held.at[q, firsts[q]], own.at[q]).start()
    for step in (2, 1, 3):
        for q in range(3):
            other = lax.rem(firsts[q] + step, 4)
            remote(
                dense_ref.at[q, pl.ds(other * 4, 4)], held.at[q, firsts[q]], send, recv.at[q],
                along(q, step),
            ).start()
    for q in range(3):
        if q == 1:
            sums[1] = take_sums(0)
        pltpu.make_async_copy(dense_ref.at[q, 0:4], held.at[q, 0], own.at[q]).wait()
        units_wait(held.at[q, 0:3], recv.at[q])

        def one(k, carry):
            place = lax.rem(seconds[q] + 1 + lax.div(k, rows // (2 * third)), 4)
            start = pl.multiple_of(lax.rem(k, rows // (2 * third)) * (2 * third), 16)
            total = held[q, 0, place, pl.ds(start, 2 * third), :].astype(F32)
            for source in range(1, 4):
                total += held[q, source, place, pl.ds(start, 2 * third), :].astype(F32)
            if q == 2:
                total = split_again(total, third)
            mids[q, place, pl.ds(start, 2 * third), :] = total.astype(BF16)
            return carry

        lax.fori_loop(0, 4 * rows // (2 * third), one, 0)
        for step in (2, 1, 3):
            other = lax.rem(seconds[q] + step, 4)
            remote(
                mids.at[q, other], lasts.at[q, seconds[q]], send2, recv2.at[q], along((q + 1) % 3, step)
            ).start()
        lasts[q, seconds[q]] = mids[q, seconds[q]]
    give_sums(1)
    for q in range(3):
        units_wait(lasts.at[q, 0:3], recv2.at[q])

        def two(j, carry):
            start = pl.multiple_of(j * 2 * third, 16)
            total = lasts[q, 0, pl.ds(start, 2 * third), :].astype(F32)
            for source in range(1, 4):
                total += lasts[q, source, pl.ds(start, 2 * third), :].astype(F32)
            acc_ref[2 * j, q * third : (q + 1) * third, :] = total[:third]
            acc_ref[2 * j + 1, q * third : (q + 1) * third, :] = total[third:]
            return carry

        lax.fori_loop(0, acc_ref.shape[0] // 2, two, 0)
    total_ref[...] = take_sums(1)
    units_wait(held.at[:, 0:3], send)
    units_wait(lasts.at[:, 0:3], send2)


def halves(x):
    high = x.astype(BF16)
    return high, (x - high.astype(F32)).astype(BF16)


def stacked(pairs):
    return jnp.concatenate([part for pair in pairs for part in pair], axis=0)


def products(lefts, right):
    n = right[0].shape[1]
    rows = lefts[0][0].shape[0]
    both = jnp.dot(stacked(lefts), jnp.concatenate(right, axis=1), preferred_element_type=F32)
    found = []
    for k in range(len(lefts)):
        high = both[2 * k * rows : (2 * k + 1) * rows]
        low = both[(2 * k + 1) * rows : (2 * k + 2) * rows]
        found.append(high[:, :n] + (high[:, n:] + low[:, :n]))
    return found


def update_kernel(count, observations, totals_ref, acc_ref, pert_ref, mean_ref, out_ref, perts, made, sems, out_sems):
    patches, fields, members, _ = pert_ref.shape

    def take(p):
        return pltpu.make_async_copy(pert_ref.at[p], perts.at[p], sems.at[p])

    def put(p):
        return pltpu.make_async_copy(made.at[p], out_ref.at[p], out_sems.at[p])

    for p in range(patches):
        take(p).start()
    base = float(members - 1) / inflation_of(totals_ref, observations)

    def one(g, carry):
        update_patches(g * count, count, fields, members, base, acc_ref, mean_ref, perts, made, take, put)
        return carry

    lax.fori_loop(0, patches // count, one, 0)
    for p in range(patches):
        put(p).wait()


def inflation_of(totals_ref, observations):
    return totals_ref[0:1, 0:1] / (totals_ref[0:1, 1:2] + float(observations))


def update_patches(first, count, fields, members, base, acc_ref, mean_ref, perts, made, take, put):
    half = members // 2
    row = lax.broadcasted_iota(jnp.int32, (members, members), 0)
    lane = lax.broadcasted_iota(jnp.int32, (members, members), 1)
    eye = jnp.where(row == lane, 1.0, 0.0)
    r = row[:half]
    c = lane[:half]
    state = []
    for q in range(count):
        packed = acc_ref[first + q, 0:half, :]
        top = jnp.where((c >= half) | (r > c), packed, 0.0)
        low = pltpu.roll(jnp.where((c < half) & (r < c), packed, 0.0), half, 1)
        part = jnp.concatenate([top, low], axis=0)
        own = jnp.sum(jnp.where(r == c, packed, 0.0), axis=0, keepdims=True)
        own = own + pltpu.roll(acc_ref[first + q, half : half + 1, :], half, 1)
        system = part + part.T + jnp.where(row == lane, own + base, 0.0)
        scaling = jnp.sqrt(jnp.sum(jnp.sum(system * system, axis=0, keepdims=True), axis=1, keepdims=True))
        root = system / scaling
        factor = 1.5 * eye - 0.5 * root
        state.append([products([halves(root)], halves(factor))[0], factor, scaling])
    for it in range(1, NS_ITERS):
        for q in range(count):
            root, inverse, _ = state[q]
            root2, inverse2 = halves(root), halves(inverse)
            factor = 1.5 * eye - 0.5 * products([inverse2], root2)[0]
            if it < NS_ITERS - 1:
                state[q][:2] = products([root2, inverse2], halves(factor))
            else:
                state[q][1] = products([inverse2], halves(factor))[0]
    for q in range(count):
        _, inverse, scaling = state[q]
        inverse = inverse * (1.0 / jnp.sqrt(scaling))
        proj = acc_ref[first + q, half + 1 : half + 2, :] + acc_ref[first + q, half + 2 : half + 3, :]
        inverse2 = halves(inverse)
        mean = jnp.broadcast_to(proj, (16, members))
        mean = products([halves(mean)], inverse2)[0]
        mean = products([halves(mean)], inverse2)[0][0:1, :]
        weights = (float(members - 1) ** 0.5 * inverse + mean).astype(BF16)
        take(first + q).wait()
        for f in range(fields):
            change = jnp.dot(weights, perts[first + q, f], preferred_element_type=F32)
            made[first + q, f] = mean_ref[first + q, f : f + 1, :] + change
        put(first + q).start()


def on_device(
    state_pert, state_mean, obs_anom, innov, obs_rinv, obs_lon, obs_lat, block_list, block_count
):
    holders = lax.axis_size(AXES)
    lon_patches, lat_patches, fields, members, columns = state_pert.shape
    patches = lon_patches * lat_patches
    list_length = block_list.shape[2]
    held_blocks, _, block_obs = obs_anom.shape
    slots = patches * list_length
    per = slots // holders
    half = members // 2

    vmem = pl.BlockSpec(memory_space=pltpu.VMEM)
    smem = pl.BlockSpec(memory_space=pltpu.SMEM)
    anywhere = pl.BlockSpec(memory_space=pl.ANY)
    wanted = block_list.reshape(slots)
    holder = wanted // held_blocks
    slot = jnp.arange(slots)
    patch = slot // list_length
    valid = (slot % list_length < jnp.repeat(block_count.reshape(patches), list_length)).astype(jnp.int32)
    patch_lon, patch_lat = patch // lat_patches, patch % lat_patches
    code = (wanted % held_blocks) * 256 + patch_lat * 128 + patch_lon * PSIDE + valid
    earlier = (holder[:, None] == holder[None, :]) & (slot[None, :] < slot[:, None])
    rank = jnp.sum(earlier.astype(jnp.int32), axis=1)
    bucket = holder * per + rank
    requests = jnp.sum(jnp.where(bucket[:, None] == slot[None, :], code[:, None], 0), axis=0)
    message = jnp.pad(requests.reshape(holders, 1, per), ((0, 0), (0, 0), (0, block_obs - per)))
    turn = 16
    codes, sums, ext = pl.pallas_call(
        functools.partial(request_kernel, turn, float(members - 1)),
        in_specs=[anywhere, vmem, vmem, vmem],
        out_specs=[vmem, vmem, vmem],
        out_shape=[
            jax.ShapeDtypeStruct((holders, 1, block_obs), jnp.int32),
            jax.ShapeDtypeStruct((8, block_obs), F32),
            jax.ShapeDtypeStruct((held_blocks, 16, block_obs), BF16),
        ],
        scratch_shapes=[
            pltpu.VMEM((held_blocks, members, block_obs), BF16),
            pltpu.VMEM((holders, 1, block_obs), jnp.int32),
            pltpu.SemaphoreType.DMA((held_blocks // turn,)),
            pltpu.SemaphoreType.DMA,
            pltpu.SemaphoreType.DMA,
        ],
        compiler_params=pltpu.CompilerParams(collective_id=2, has_side_effects=True),
        name="requests",
    )(obs_anom, obs_rinv, innov, message)
    third = (half + 8) // 3
    short = codes.reshape(holders, block_obs)[:, :8].reshape(holders * 8)
    starts = (((short >> 4) & 7) * lat_patches + ((short >> 7) & 1)) * third
    got, tables, lines = pl.pallas_call(
        functools.partial(gram_kernel, per, lon_patches, lat_patches),
        in_specs=[smem, anywhere, anywhere, anywhere, vmem, vmem, vmem, vmem],
        out_specs=[anywhere] * 3,
        out_shape=[
            jax.ShapeDtypeStruct((3, 8, 16, per * third, members), BF16),
            jax.ShapeDtypeStruct((3, 8, 8, 128), jnp.int32),
            jax.ShapeDtypeStruct((8, 8, block_obs), F32),
        ],
        scratch_shapes=[
            pltpu.VMEM((holders, 3, per * third, members), BF16),
            pltpu.VMEM((held_blocks, members, block_obs), BF16),
            pltpu.SemaphoreType.DMA((held_blocks // turn,)),
            pltpu.SemaphoreType.DMA,
            pltpu.SemaphoreType.DMA,
            pltpu.SemaphoreType.DMA,
            pltpu.SemaphoreType.DMA,
            pltpu.SemaphoreType.DMA,
            pltpu.SemaphoreType.DMA((3,)),
            pltpu.SemaphoreType.DMA,
            pltpu.SemaphoreType.DMA,
            pltpu.SemaphoreType.DMA,
        ],
        compiler_params=pltpu.CompilerParams(collective_id=0, has_side_effects=True),
        name="grams",
    )(codes.reshape(holders * block_obs), starts.reshape(8, 128), sums, obs_anom, ext, obs_rinv, obs_lon, obs_lat)

    dense = pl.pallas_call(
        functools.partial(add_kernel, per),
        in_specs=[smem, anywhere],
        out_specs=anywhere,
        out_shape=jax.ShapeDtypeStruct((3, 16, patches * third, members), BF16),
        scratch_shapes=[
            pltpu.VMEM((3, 8, 16, per * third, members), BF16),
            pltpu.VMEM((3, 16, patches * third, members), BF16),
            pltpu.SemaphoreType.DMA((3, 8)),
            pltpu.SemaphoreType.DMA((3,)),
        ]
        + [pltpu.VMEM((patches * third, members), F32)] * CHAINS,
        name="adds",
    )(tables.reshape(3 * 8 * 1024), got)

    acc, totals = pl.pallas_call(
        plane_kernel,
        in_specs=[anywhere, vmem],
        out_specs=[vmem, vmem],
        out_shape=[
            jax.ShapeDtypeStruct((patches, half + 8, members), F32),
            jax.ShapeDtypeStruct((8, block_obs), F32),
        ],
        scratch_shapes=[
            pltpu.VMEM((3, 4, 4, patches * third, members), BF16),
            pltpu.VMEM((3, 4, patches * third, members), BF16),
            pltpu.VMEM((3, 4, patches * third, members), BF16),
            pltpu.VMEM((2, 8, block_obs), F32),
            pltpu.VMEM((2, 4, 8, block_obs), F32),
            pltpu.SemaphoreType.DMA,
            pltpu.SemaphoreType.DMA((3,)),
            pltpu.SemaphoreType.DMA,
            pltpu.SemaphoreType.DMA((3,)),
            pltpu.SemaphoreType.DMA((3,)),
            pltpu.SemaphoreType.DMA((2,)),
            pltpu.SemaphoreType.DMA((2,)),
        ],
        compiler_params=pltpu.CompilerParams(collective_id=1, has_side_effects=True),
        name="planes",
    )(dense, lines)

    updated = pl.pallas_call(
        functools.partial(update_kernel, PAIR, holders * held_blocks * block_obs),
        in_specs=[vmem, vmem, anywhere, vmem],
        out_specs=anywhere,
        out_shape=jax.ShapeDtypeStruct((patches, fields, members, columns), F32),
        scratch_shapes=[
            pltpu.VMEM((patches, fields, members, columns), BF16),
            pltpu.VMEM((patches, fields, members, columns), F32),
            pltpu.SemaphoreType.DMA((patches,)),
            pltpu.SemaphoreType.DMA((patches,)),
        ],
        name="update",
    )(
        totals,
        acc,
        state_pert.reshape(patches, fields, members, columns),
        state_mean.reshape(patches, fields, columns),
    )
    return updated.reshape(lon_patches, lat_patches, fields, members, columns)


def solution(mesh):
    in_specs = (
        P("lon", "lat", None, None, None),
        P("lon", "lat", None, None),
        P(AXES, None, None),
        P(AXES, None),
        P(AXES, None),
        P(AXES, None),
        P(AXES, None),
        P("lon", "lat", None),
        P("lon", "lat"),
    )
    out_specs = P("lon", "lat", None, None, None)
    return jax.shard_map(
        on_device, mesh=mesh, in_specs=in_specs, out_specs=out_specs, check_vma=False
    )
```

```python
import functools

import jax
import jax.numpy as jnp
from jax import lax
from jax.experimental import pallas as pl
from jax.experimental.pallas import tpu as pltpu
from jax.sharding import PartitionSpec as P

PSIDE = 16
NS_ITERS = 5
LOC_SCALE = 48.0
AXES = ("lon", "lat")
MESH = pl.DeviceIdType.MESH
CHAINS = 2
PAIR = 8
F32 = jnp.float32
BF16 = jnp.bfloat16


def request_kernel(turn, members_less, anom_ref, rinv_ref, innov_ref, ask_ref, codes_ref, sums_ref, ext_ref, held,
                   mid, row_in, sems, send, recv, send2, recv2):
    blocks, _, width = anom_ref.shape
    turns = blocks // turn
    lats, lons = ask_ref.shape[0:2]
    lon, lat = lax.axis_index("lon"), lax.axis_index("lat")

    def copy(k):
        return pltpu.make_async_copy(
            anom_ref.at[pl.ds(k * turn, turn)], held.at[pl.ds(k * turn, turn)], sems.at[k]
        )

    barrier = pltpu.get_barrier_semaphore()
    on_lat = [lax.rem(lat + step, lats) for step in range(1, lats)]
    on_lon = [lax.rem(lon + step, lons) for step in range(1, lons)]
    for device in [(lon, other) for other in on_lat] + [(other, lat) for other in on_lon]:
        pl.semaphore_signal(barrier, inc=1, device_id=device, device_id_type=MESH)
    for k in range(turns):
        copy(k).start()
    mid[lat] = ask_ref[lat]
    pl.semaphore_wait(barrier, lats + lons - 2)

    def send_rows(src, dst, sent, got, device):
        pltpu.make_async_remote_copy(
            src_ref=src, dst_ref=dst, send_sem=sent, recv_sem=got, device_id=device, device_id_type=MESH
        ).start()

    for other in on_lat:
        send_rows(ask_ref.at[other], mid.at[lat], send, recv, (lon, other))
    innov = innov_ref[...]
    high = innov.astype(BF16).astype(F32)
    rest = innov - high
    middle = rest.astype(BF16).astype(F32)
    ext = jnp.concatenate(
        [high[:, None, :], middle[:, None, :], (rest - middle)[:, None, :], jnp.zeros((blocks, 13, width), F32)],
        axis=1,
    )
    ext_ref[...] = ext.astype(BF16)
    first = jnp.sum((rinv_ref[...] * innov * innov).reshape(blocks // 8, 8, width), axis=0)
    units_wait(mid.at[0 : lats - 1], recv)
    for other in on_lon:
        send_rows(mid.at[:, other], row_in.at[lon], send2, recv2, (other, lat))
    row_in[lon] = mid[:, lon]

    def one(k, total):
        copy(k).wait()
        start = pl.multiple_of(k * turn, turn)
        rinv = rinv_ref[pl.ds(start, turn), :]
        for b in range(turn):
            a = held[start + b].astype(F32)
            squares = jnp.sum((a * a).reshape(-1, 8, width), axis=0)
            total = total + squares * rinv[b : b + 1, :]
        return total

    second = lax.fori_loop(0, turns, one, jnp.zeros((8, width), F32))

    def whole(x):
        return jnp.sum(jnp.sum(x, axis=0, keepdims=True), axis=1, keepdims=True)

    lane = lax.broadcasted_iota(jnp.int32, (8, width), 1)
    sums_ref[...] = jnp.where(
        lane == 0, whole(first), jnp.where(lane == 1, whole(second) / members_less, 0.0)
    )
    units_wait(mid.at[0 : lats - 1], send)
    units_wait(row_in.at[0 : lons - 1], send2)
    units_wait(row_in.at[0 : lons - 1], recv2)
    codes_ref[...] = row_in[...]


def coordinates():
    lon, lat = lax.axis_index("lon"), lax.axis_index("lat")
    return lax.div(lat, 4), lax.div(lon, 2), lax.rem(lat, 4), lax.rem(lon, 2)


def device_at(x, y, z, core):
    return (y * 2 + core, x * 4 + z)


def units_wait(ref, sem):
    pltpu.make_async_copy(ref, ref, sem).wait()


LINE_PEERS = [(0, 0, 0, 1)] + [
    tuple(step if axis == a else 0 for a in range(3)) + (core,)
    for axis in range(3)
    for step in (1, 2, 3)
    for core in (0, 1)
]
AXIS_PEERS = [
    tuple(step if axis == a else 0 for a in range(3)) + (0,) for axis in range(3) for step in (1, 2, 3)
]


def shifted(me, offset):
    x, y, z, core = me
    dx, dy, dz, dc = offset
    return tuple(
        lax.rem(a + d, n) if not isinstance(d, int) or d else a
        for a, d, n in ((x, dx, 4), (y, dy, 4), (z, dz, 4), (core, dc, 2))
    )


def greet(me, offsets):
    barrier = pltpu.get_barrier_semaphore()
    for offset in offsets:
        pl.semaphore_signal(
            barrier, inc=1, device_id=device_at(*shifted(me, offset)), device_id_type=MESH
        )
    pl.semaphore_wait(barrier, len(offsets))


def remote(src, dst, send, recv, target):
    return pltpu.make_async_remote_copy(
        src_ref=src,
        dst_ref=dst,
        send_sem=send,
        recv_sem=recv,
        device_id=device_at(*target),
        device_id_type=MESH,
    )


def gram_kernel(per, lon_patches, lat_patches, code_ref, table_ref, sums_ref, anom_ref, ext_ref, rinv_ref,
                lon_ref, lat_ref, got_ref, codes_ref, lines_ref, stage, blocks, block_sems, send, recv, own,
                send2, recv2, own2, send3, recv3, own3):
    me = coordinates()
    xm, ym, zm, cm = me
    mine = (zm, xm, ym)
    chunks = block_sems.shape[0]
    turn = anom_ref.shape[0] // chunks
    members = anom_ref.shape[1]
    half = members // 2
    third = (half + 8) // 3
    requesters = stage.shape[0]
    grid_lon = float(8 * lon_patches * PSIDE)
    row = lax.broadcasted_iota(jnp.int32, (half, members), 0)
    lane = lax.broadcasted_iota(jnp.int32, (half, members), 1)
    keep = (lane >= half) | (row >= lane)
    on_diag = row == lane
    row8 = lax.broadcasted_iota(jnp.int32, (8, members), 0)

    def fetch(k):
        part = pl.ds(k * turn, turn)
        return pltpu.make_async_copy(anom_ref.at[part], blocks.at[part], block_sems.at[k])

    for k in range(chunks):
        fetch(k).start()
    greet(me, LINE_PEERS)
    for q in range(3):
        source = mine[q] * 2 + cm
        for step in range(4):
            for core in range(2):
                offset = [0, 0, 0, core]
                offset[(2, 0, 1)[q]] = step
                dst = codes_ref.at[q, source]
                if step == 0 and core == 0:
                    pltpu.make_async_copy(table_ref, dst, own2.at[q]).start()
                else:
                    remote(table_ref, dst, send2, recv2, shifted(me, offset)).start()
                if q == 0:
                    line = lines_ref.at[source]
                    if step == 0 and core == 0:
                        pltpu.make_async_copy(sums_ref, line, own3).start()
                    else:
                        remote(sums_ref, line, send3, recv3, shifted(me, offset)).start()

    for k in range(chunks):
        fetch(k).wait()

    def offset_of(i):
        dx = lax.rem(i, 4)
        dy = lax.rem(i + lax.div(i, 4), 4)
        dz = lax.rem(i + lax.div(i, 16), 4)
        return dx, dy, dz, lax.div(i, 64)

    def ship(i):
        dx, dy, dz, dc = offset_of(i)
        x, y, z, core = shifted(me, (dx, dy, dz, dc))
        targets = ((xm, ym, z, core), (x, ym, zm, core), (xm, y, zm, core))
        places = (x * 4 + y, y * 4 + z, z * 4 + x)
        for q, moved in enumerate((dz, dx, dy)):
            src = stage.at[i, q]
            dst = got_ref.at[q, mine[q] * 2 + cm, places[q]]
            stays = (moved == 0) & (dc == 0)

            @pl.when(stays)
            def _():
                pltpu.make_async_copy(src, dst, own).start()

            @pl.when(jnp.logical_not(stays))
            def _():
                remote(src, dst, send, recv, targets[q]).start()

    def one(i, carry):
        x, y, z, core = shifted(me, offset_of(i))
        lon_device = y * 2 + core
        lat_device = x * 4 + z
        who8 = (lon_device * 16 + lat_device) * members
        lon_first = lon_device * (lon_patches * PSIDE)
        lat_first = lat_device * (lat_patches * PSIDE)
        pieces = []
        for s in range(per):
            code = code_ref[who8 + s]
            valid = code & 1
            held = code >> 8
            cl = (lon_first + (code & 112)).astype(F32) + (PSIDE - 1) / 2.0
            ct = (lat_first + ((code & 128) >> 3)).astype(F32) + (PSIDE - 1) / 2.0
            gap = jnp.abs(lon_ref[pl.ds(held, 1), :].astype(F32) - cl)
            gap = jnp.minimum(gap, grid_lon - gap)
            other = lat_ref[pl.ds(held, 1), :].astype(F32) - ct
            weight = rinv_ref[pl.ds(held, 1), :] * jnp.exp(
                -(gap * gap + other * other) / (2.0 * LOC_SCALE * LOC_SCALE)
            )
            weight = weight * valid.astype(F32)
            a = blocks[held]
            scaled = (a.astype(F32) * weight).astype(BF16)
            left = jnp.concatenate([a, ext_ref[held]], axis=0)
            full = lax.dot_general(
                left, scaled, (((1,), (1,)), ((), ())), preferred_element_type=F32
            )
            top = full[:half, :]
            low = pltpu.roll(full[half:members, :], half, 1)
            diag = jnp.sum(jnp.where(on_diag, low, 0.0), axis=0, keepdims=True)
            proj = jnp.sum(full[members : members + 8, :], axis=0, keepdims=True)
            high = proj.astype(BF16).astype(F32)
            extra = jnp.where(
                row8 == 0, diag, jnp.where(row8 == 1, high, jnp.where(row8 == 2, proj - high, 0.0))
            )
            pieces.append(jnp.concatenate([jnp.where(keep, top, low), extra], axis=0))
        for q in range(3):
            for s in range(0, per, 2):
                both = jnp.concatenate(
                    [pieces[s][q * third : (q + 1) * third], pieces[s + 1][q * third : (q + 1) * third]],
                    axis=0,
                )
                stage[i, q, s * third : (s + 2) * third, :] = both.astype(BF16)

        @pl.when(i > 0)
        def _():
            ship(i - 1)

        return carry

    lax.fori_loop(0, requesters, one, 0)
    ship(jnp.int32(requesters - 1))

    for q in range(3):
        pltpu.make_async_copy(table_ref, codes_ref.at[q, 0], own2.at[q]).wait()
    pltpu.make_async_copy(sums_ref, lines_ref.at[0], own3).wait()
    units_wait(lines_ref.at[0:7], send3)
    units_wait(lines_ref.at[0:7], recv3)
    units_wait(codes_ref.at[:, 0:7], send2)
    units_wait(codes_ref.at[:, 0:7], recv2)
    units_wait(stage.at[0:16], own)
    units_wait(stage.at[0:112], send)
    units_wait(got_ref.at[:, 0:7], recv)


def split_again(total, third):
    row8 = lax.broadcasted_iota(jnp.int32, (8, total.shape[1]), 0)
    parts = []
    for t in range(2):
        top = total[t * third : t * third + 16]
        last = total[t * third + 16 : (t + 1) * third]
        proj = last[1:2, :] + last[2:3, :]
        high = proj.astype(BF16).astype(F32)
        parts += [top, jnp.where(row8 == 1, high, jnp.where(row8 == 2, proj - high, last))]
    return jnp.concatenate(parts, axis=0)


def add_kernel(per, starts_ref, got_ref, out_ref, held, made, sems, out_sems, *accs):
    sources, places = held.shape[1:3]
    third = held.shape[3] // per
    chains = len(accs)
    xm, ym, zm, cm = coordinates()

    def copy(q, source):
        return pltpu.make_async_copy(got_ref.at[q, source], held.at[q, source], sems.at[q, source])

    for q in range(3):
        for source in range(sources):
            copy(q, source).start()
    for q in range(3):
        for source in range(sources):
            copy(q, source).wait()

        def one(place, carry):
            major, minor = lax.div(place, 4), lax.rem(place, 4)
            x = (major, xm, minor)[q]
            y = (minor, major, ym)[q]
            z = (zm, minor, major)[q]
            first = ((y * 2 + cm) * 16 + x * 4 + z) * 8
            for acc in accs:
                acc[...] = jnp.zeros_like(acc)
            for source in range(sources):
                for s in range(0, per, 2):
                    both = held[q, source, place, s * third : (s + 2) * third, :].astype(F32)
                    for t in range(2):
                        start = pl.multiple_of(starts_ref[first + ((q * sources + source) * 1024 + s + t)], 8)
                        accs[(s + t) % chains][pl.ds(start, third), :] += both[t * third : (t + 1) * third]
            if q < 2:
                made[q, place] = functools.reduce(lambda a, b: a + b, [acc[...] for acc in accs]).astype(BF16)
            else:
                for p in range(0, accs[0].shape[0] // third, 2):
                    rows = slice(p * third, (p + 2) * third)
                    total = functools.reduce(lambda a, b: a + b, [acc[rows, :] for acc in accs])
                    made[q, place, rows, :] = split_again(total, third).astype(BF16)
            return carry

        lax.fori_loop(0, places, one, 0)
        pltpu.make_async_copy(made.at[q], out_ref.at[q], out_sems.at[q]).start()
    for q in range(3):
        pltpu.make_async_copy(made.at[q], out_ref.at[q], out_sems.at[q]).wait()


def plane_kernel(dense_ref, lines_ref, acc_ref, total_ref, held, mids, lasts, sums, parts, send, recv, send2, recv2,
                 own, send3, recv3):
    me = coordinates()
    xm, ym, zm, _ = me
    firsts, seconds = (xm, ym, zm), (ym, zm, xm)
    rows = dense_ref.shape[2]
    third = rows // acc_ref.shape[0]

    def along(axis, step):
        return shifted(me, tuple(step if a == axis else 0 for a in range(3)) + (0,))

    def give_sums(axis):
        here = (xm, ym)[axis]
        for step in (2, 1, 3):
            remote(sums.at[axis], parts.at[axis, here], send3.at[axis], recv3.at[axis], along(axis, step)).start()
        parts[axis, here] = sums[axis]

    def take_sums(axis):
        units_wait(parts.at[axis, 0:3], send3.at[axis])
        units_wait(parts.at[axis, 0:3], recv3.at[axis])
        return jnp.sum(parts[axis], axis=0)

    sums[0] = jnp.sum(lines_ref[...], axis=0)
    greet(me, AXIS_PEERS)
    give_sums(0)
    for q in range(3):
        mine = dense_ref.at[q, pl.ds(firsts[q] * 4, 4)]
        pltpu.make_async_copy(mine, held.at[q, firsts[q]], own.at[q]).start()
    for step in (2, 1, 3):
        for q in range(3):
            other = lax.rem(firsts[q] + step, 4)
            remote(
                dense_ref.at[q, pl.ds(other * 4, 4)], held.at[q, firsts[q]], send, recv.at[q],
                along(q, step),
            ).start()
    for q in range(3):
        if q == 1:
            sums[1] = take_sums(0)
        pltpu.make_async_copy(dense_ref.at[q, 0:4], held.at[q, 0], own.at[q]).wait()
        units_wait(held.at[q, 0:3], recv.at[q])

        def one(k, carry):
            place = lax.rem(seconds[q] + 1 + lax.div(k, rows // (2 * third)), 4)
            start = pl.multiple_of(lax.rem(k, rows // (2 * third)) * (2 * third), 16)
            total = held[q, 0, place, pl.ds(start, 2 * third), :].astype(F32)
            for source in range(1, 4):
                total += held[q, source, place, pl.ds(start, 2 * third), :].astype(F32)
            if q == 2:
                total = split_again(total, third)
            mids[q, place, pl.ds(start, 2 * third), :] = total.astype(BF16)
            return carry

        lax.fori_loop(0, 4 * rows // (2 * third), one, 0)
        for step in (2, 1, 3):
            other = lax.rem(seconds[q] + step, 4)
            remote(
                mids.at[q, other], lasts.at[q, seconds[q]], send2, recv2.at[q], along((q + 1) % 3, step)
            ).start()
        lasts[q, seconds[q]] = mids[q, seconds[q]]
    give_sums(1)
    for q in range(3):
        units_wait(lasts.at[q, 0:3], recv2.at[q])

        def two(j, carry):
            start = pl.multiple_of(j * 2 * third, 16)
            total = lasts[q, 0, pl.ds(start, 2 * third), :].astype(F32)
            for source in range(1, 4):
                total += lasts[q, source, pl.ds(start, 2 * third), :].astype(F32)
            acc_ref[2 * j, q * third : (q + 1) * third, :] = total[:third]
            acc_ref[2 * j + 1, q * third : (q + 1) * third, :] = total[third:]
            return carry

        lax.fori_loop(0, acc_ref.shape[0] // 2, two, 0)
    total_ref[...] = take_sums(1)
    units_wait(held.at[:, 0:3], send)
    units_wait(lasts.at[:, 0:3], send2)


def halves(x):
    high = x.astype(BF16)
    return high, (x - high.astype(F32)).astype(BF16)


def stacked(pairs):
    return jnp.concatenate([part for pair in pairs for part in pair], axis=0)


def products(lefts, right):
    n = right[0].shape[1]
    rows = lefts[0][0].shape[0]
    both = jnp.dot(stacked(lefts), jnp.concatenate(right, axis=1), preferred_element_type=F32)
    found = []
    for k in range(len(lefts)):
        high = both[2 * k * rows : (2 * k + 1) * rows]
        low = both[(2 * k + 1) * rows : (2 * k + 2) * rows]
        found.append(high[:, :n] + (high[:, n:] + low[:, :n]))
    return found


def update_kernel(count, observations, totals_ref, acc_ref, pert_ref, mean_ref, out_ref, perts, made, sems, out_sems):
    patches, fields, members, _ = pert_ref.shape

    def take(p):
        return pltpu.make_async_copy(pert_ref.at[p], perts.at[p], sems.at[p])

    def put(p):
        return pltpu.make_async_copy(made.at[p], out_ref.at[p], out_sems.at[p])

    for p in range(patches):
        take(p).start()
    base = float(members - 1) / inflation_of(totals_ref, observations)

    def one(g, carry):
        update_patches(g * count, count, fields, members, base, acc_ref, mean_ref, perts, made, take, put)
        return carry

    lax.fori_loop(0, patches // count, one, 0)
    for p in range(patches):
        put(p).wait()


def inflation_of(totals_ref, observations):
    return totals_ref[0:1, 0:1] / (totals_ref[0:1, 1:2] + float(observations))


def update_patches(first, count, fields, members, base, acc_ref, mean_ref, perts, made, take, put):
    half = members // 2
    row = lax.broadcasted_iota(jnp.int32, (members, members), 0)
    lane = lax.broadcasted_iota(jnp.int32, (members, members), 1)
    eye = jnp.where(row == lane, 1.0, 0.0)
    r = row[:half]
    c = lane[:half]
    state = []
    for q in range(count):
        packed = acc_ref[first + q, 0:half, :]
        top = jnp.where((c >= half) | (r > c), packed, 0.0)
        low = pltpu.roll(jnp.where((c < half) & (r < c), packed, 0.0), half, 1)
        part = jnp.concatenate([top, low], axis=0)
        own = jnp.sum(jnp.where(r == c, packed, 0.0), axis=0, keepdims=True)
        own = own + pltpu.roll(acc_ref[first + q, half : half + 1, :], half, 1)
        system = part + part.T + jnp.where(row == lane, own + base, 0.0)
        scaling = jnp.sqrt(jnp.sum(jnp.sum(system * system, axis=0, keepdims=True), axis=1, keepdims=True))
        root = system / scaling
        factor = 1.5 * eye - 0.5 * root
        state.append([products([halves(root)], halves(factor))[0], factor, scaling])
    for it in range(1, NS_ITERS):
        for q in range(count):
            root, inverse, _ = state[q]
            root2, inverse2 = halves(root), halves(inverse)
            factor = 1.5 * eye - 0.5 * products([inverse2], root2)[0]
            if it < NS_ITERS - 1:
                state[q][:2] = products([root2, inverse2], halves(factor))
            else:
                state[q][1] = products([inverse2], halves(factor))[0]
    for q in range(count):
        _, inverse, scaling = state[q]
        inverse = inverse * (1.0 / jnp.sqrt(scaling))
        proj = acc_ref[first + q, half + 1 : half + 2, :] + acc_ref[first + q, half + 2 : half + 3, :]
        inverse2 = halves(inverse)
        mean = jnp.broadcast_to(proj, (16, members))
        mean = products([halves(mean)], inverse2)[0]
        mean = products([halves(mean)], inverse2)[0][0:1, :]
        weights = (float(members - 1) ** 0.5 * inverse + mean).astype(BF16)
        take(first + q).wait()
        for f in range(fields):
            change = jnp.dot(weights, perts[first + q, f], preferred_element_type=F32)
            made[first + q, f] = mean_ref[first + q, f : f + 1, :] + change
        put(first + q).start()


def on_device(
    state_pert, state_mean, obs_anom, innov, obs_rinv, obs_lon, obs_lat, block_list, block_count
):
    holders = lax.axis_size(AXES)
    lon_patches, lat_patches, fields, members, columns = state_pert.shape
    patches = lon_patches * lat_patches
    list_length = block_list.shape[2]
    held_blocks, _, block_obs = obs_anom.shape
    slots = patches * list_length
    per = slots // holders
    half = members // 2

    vmem = pl.BlockSpec(memory_space=pltpu.VMEM)
    smem = pl.BlockSpec(memory_space=pltpu.SMEM)
    anywhere = pl.BlockSpec(memory_space=pl.ANY)
    wanted = block_list.reshape(slots)
    holder = wanted // held_blocks
    slot = jnp.arange(slots)
    patch = slot // list_length
    valid = (slot % list_length < jnp.repeat(block_count.reshape(patches), list_length)).astype(jnp.int32)
    patch_lon, patch_lat = patch // lat_patches, patch % lat_patches
    code = (wanted % held_blocks) * 256 + patch_lat * 128 + patch_lon * PSIDE + valid
    earlier = (holder[:, None] == holder[None, :]) & (slot[None, :] < slot[:, None])
    rank = jnp.sum(earlier.astype(jnp.int32), axis=1)
    bucket = holder * per + rank
    requests = jnp.sum(jnp.where(bucket[:, None] == slot[None, :], code[:, None], 0), axis=0)
    lons, lats = lax.axis_size("lon"), lax.axis_size("lat")
    message = jnp.pad(
        requests.reshape(lons, lats, 1, per).swapaxes(0, 1), ((0, 0), (0, 0), (0, 0), (0, block_obs - per))
    )
    turn = 16
    codes, sums, ext = pl.pallas_call(
        functools.partial(request_kernel, turn, float(members - 1)),
        in_specs=[anywhere, vmem, vmem, vmem],
        out_specs=[vmem, vmem, vmem],
        out_shape=[
            jax.ShapeDtypeStruct((lons, lats, 1, block_obs), jnp.int32),
            jax.ShapeDtypeStruct((8, block_obs), F32),
            jax.ShapeDtypeStruct((held_blocks, 16, block_obs), BF16),
        ],
        scratch_shapes=[
            pltpu.VMEM((held_blocks, members, block_obs), BF16),
            pltpu.VMEM((lats, lons, 1, block_obs), jnp.int32),
            pltpu.VMEM((lons, lats, 1, block_obs), jnp.int32),
            pltpu.SemaphoreType.DMA((held_blocks // turn,)),
            pltpu.SemaphoreType.DMA,
            pltpu.SemaphoreType.DMA,
            pltpu.SemaphoreType.DMA,
            pltpu.SemaphoreType.DMA,
        ],
        compiler_params=pltpu.CompilerParams(collective_id=2, has_side_effects=True),
        name="requests",
    )(obs_anom, obs_rinv, innov, message)
    third = (half + 8) // 3
    short = codes.reshape(holders, block_obs)[:, :8].reshape(holders * 8)
    starts = (((short >> 4) & 7) * lat_patches + ((short >> 7) & 1)) * third
    got, tables, lines = pl.pallas_call(
        functools.partial(gram_kernel, per, lon_patches, lat_patches),
        in_specs=[smem, anywhere, anywhere, anywhere, vmem, vmem, vmem, vmem],
        out_specs=[anywhere] * 3,
        out_shape=[
            jax.ShapeDtypeStruct((3, 8, 16, per * third, members), BF16),
            jax.ShapeDtypeStruct((3, 8, 8, 128), jnp.int32),
            jax.ShapeDtypeStruct((8, 8, block_obs), F32),
        ],
        scratch_shapes=[
            pltpu.VMEM((holders, 3, per * third, members), BF16),
            pltpu.VMEM((held_blocks, members, block_obs), BF16),
            pltpu.SemaphoreType.DMA((held_blocks // turn,)),
            pltpu.SemaphoreType.DMA,
            pltpu.SemaphoreType.DMA,
            pltpu.SemaphoreType.DMA,
            pltpu.SemaphoreType.DMA,
            pltpu.SemaphoreType.DMA,
            pltpu.SemaphoreType.DMA((3,)),
            pltpu.SemaphoreType.DMA,
            pltpu.SemaphoreType.DMA,
            pltpu.SemaphoreType.DMA,
        ],
        compiler_params=pltpu.CompilerParams(collective_id=0, has_side_effects=True),
        name="grams",
    )(codes.reshape(holders * block_obs), starts.reshape(8, 128), sums, obs_anom, ext, obs_rinv, obs_lon, obs_lat)

    dense = pl.pallas_call(
        functools.partial(add_kernel, per),
        in_specs=[smem, anywhere],
        out_specs=anywhere,
        out_shape=jax.ShapeDtypeStruct((3, 16, patches * third, members), BF16),
        scratch_shapes=[
            pltpu.VMEM((3, 8, 16, per * third, members), BF16),
            pltpu.VMEM((3, 16, patches * third, members), BF16),
            pltpu.SemaphoreType.DMA((3, 8)),
            pltpu.SemaphoreType.DMA((3,)),
        ]
        + [pltpu.VMEM((patches * third, members), F32)] * CHAINS,
        name="adds",
    )(tables.reshape(3 * 8 * 1024), got)

    acc, totals = pl.pallas_call(
        plane_kernel,
        in_specs=[anywhere, vmem],
        out_specs=[vmem, vmem],
        out_shape=[
            jax.ShapeDtypeStruct((patches, half + 8, members), F32),
            jax.ShapeDtypeStruct((8, block_obs), F32),
        ],
        scratch_shapes=[
            pltpu.VMEM((3, 4, 4, patches * third, members), BF16),
            pltpu.VMEM((3, 4, patches * third, members), BF16),
            pltpu.VMEM((3, 4, patches * third, members), BF16),
            pltpu.VMEM((2, 8, block_obs), F32),
            pltpu.VMEM((2, 4, 8, block_obs), F32),
            pltpu.SemaphoreType.DMA,
            pltpu.SemaphoreType.DMA((3,)),
            pltpu.SemaphoreType.DMA,
            pltpu.SemaphoreType.DMA((3,)),
            pltpu.SemaphoreType.DMA((3,)),
            pltpu.SemaphoreType.DMA((2,)),
            pltpu.SemaphoreType.DMA((2,)),
        ],
        compiler_params=pltpu.CompilerParams(collective_id=1, has_side_effects=True),
        name="planes",
    )(dense, lines)

    updated = pl.pallas_call(
        functools.partial(update_kernel, PAIR, holders * held_blocks * block_obs),
        in_specs=[vmem, vmem, anywhere, vmem],
        out_specs=anywhere,
        out_shape=jax.ShapeDtypeStruct((patches, fields, members, columns), F32),
        scratch_shapes=[
            pltpu.VMEM((patches, fields, members, columns), BF16),
            pltpu.VMEM((patches, fields, members, columns), F32),
            pltpu.SemaphoreType.DMA((patches,)),
            pltpu.SemaphoreType.DMA((patches,)),
        ],
        name="update",
    )(
        totals,
        acc,
        state_pert.reshape(patches, fields, members, columns),
        state_mean.reshape(patches, fields, columns),
    )
    return updated.reshape(lon_patches, lat_patches, fields, members, columns)


def solution(mesh):
    in_specs = (
        P("lon", "lat", None, None, None),
        P("lon", "lat", None, None),
        P(AXES, None, None),
        P(AXES, None),
        P(AXES, None),
        P(AXES, None),
        P(AXES, None),
        P("lon", "lat", None),
        P("lon", "lat"),
    )
    out_specs = P("lon", "lat", None, None, None)
    return jax.shard_map(
        on_device, mesh=mesh, in_specs=in_specs, out_specs=out_specs, check_vma=False
    )
```
